128 devices in a mesh: gx: 4 (over x), gy: 4 (over y), gz: 8 (over z, core).
Axes of the slice: x: 4, y: 4, z: 4, core: 2. Of those that a mesh axis runs over, the one named last changes fastest.
Arguments:
- fields: bfloat16 [16384, 2048], P(('gx', 'gy', 'gz')), may hold values from -6 to 6
- coordinates: float32 [3, 2097152], P(None, ('gx', 'gy', 'gz')), may hold values from -1 to 1
- element_rank: int32 [2097152, 1], P(('gx', 'gy', 'gz')), may hold values from 0 to 127; in each aligned block of 16384 rows (0 to 16383, 16384 to 32767, ...) at most 160 rows name the same one
- element_slot: int32 [2097152], P(('gx', 'gy', 'gz')), may hold values from 0 to 127
Outputs:
- samples: float32 [4, 2097152], P(None, ('gx', 'gy', 'gz'))
The draws below stay inside these ranges and needn't reach their ends.
Inputs may be any that keep to these rules, and one draw needn't show every extreme that they name: `element_rank`: among the probes of one device no rank is named by more than 160 probes, and in some devices' blocks one rank is named by exactly 160.
All inputs are finite; a program needn't handle non-finite values.
Results may differ from the reference program's by a relative error of at most 0.0024.
Values sent between devices are 32-bit elements; how exact they have to be, the bound alone decides.
A program may use at most 64 MiB of HBM per device.

```python
import math
import jax
import jax.numpy as jnp
import numpy as np
from jax import lax

ROW = 2048
E_DEV = 128
P_DEV = 16384
CAP = 160
ELEMENTS = 16384
PROBES = 2097152
DEVICES = 128


def place_ends(values, key, least, largest):
    longest = values.shape.index(max(values.shape))
    spots = []
    for shift in (0, 1):
        where = [jax.random.randint(jax.random.fold_in(key, axis), (), 0, length) for axis, length in enumerate(values.shape)]
        where[longest] = (where[longest] + shift) % values.shape[longest]
        spots.append(tuple(where))
    return values.at[spots[0]].set(least).at[spots[1]].set(largest)


def shard_levels(rng, dims, split, least, largest):
    loudness = 1.0
    for axis_at, parts in split:
        heights = jax.random.uniform(jax.random.fold_in(jax.random.fold_in(rng, 6), axis_at), (parts,), jnp.float32, least / len(split), largest / len(split))
        loudness = loudness * jnp.repeat(jnp.exp(heights), dims[axis_at] // parts).reshape((-1,) + (1,) * (len(dims) - 1 - axis_at))
    return loudness


def routed_block(key, own, number, rows, count, top, most, slope):
    sequence = jax.random.permutation(key, count)
    packed, usual = shares(count, rows * top, most, slope, True), shares(count, rows * top, most, slope, False)
    places = jnp.arange(count)

    def named(sizes, turn):
        used = int((sizes > 0).sum())
        fixed = max(1, used // 4)
        shifted = fixed + (places - fixed + turn * (used - fixed)) % max(1, count - fixed)
        return jnp.zeros((count,), jnp.int32).at[sequence[jnp.where(places < fixed, places, shifted)]].set(jnp.asarray(sizes, jnp.int32))

    sizes = jnp.where(number % 4 == 0, named(packed, number // 4), named(usual, number - number // 4 - 1))
    mixed = jax.random.permutation(jax.random.fold_in(own, 3), count)
    source_of, sink = mixed[0:count // 2 * 2:2], mixed[1:count // 2 * 2:2]
    margin = jnp.minimum(sizes[source_of] - 1, most - sizes[sink]) // 2
    margin = jnp.where((source_of == sequence[0]) | (sink == sequence[0]) | (sizes[sink] == 0), 0, jnp.maximum(margin, 0))
    shifted = jax.random.randint(jax.random.fold_in(own, 4), (count // 2,), 0, 1 << 20) % (margin + 1)
    sizes = sizes.at[source_of].add(-shifted).at[sink].add(shifted)
    labels = jnp.searchsorted(jnp.cumsum(sizes), jnp.arange(rows * top), side="right").astype(jnp.int32)
    listing = labels.reshape(top, rows).T
    listing = listing[jax.random.permutation(jax.random.fold_in(own, 1), rows)]
    turn = jax.random.randint(jax.random.fold_in(own, 2), (rows, 1), 0, top)
    return jnp.take_along_axis(listing, (jnp.arange(top)[None, :] + turn) % top, axis=1)


def shares(count, total, bound, skew, full):
    loads = [(1 << 20) // math.isqrt(standing ** skew) + 1 for standing in range(1, count + 1)]
    largest = bound if full else min(bound, max(-(-total // count), total * loads[0] // sum(loads)))
    least = 1 if total - largest >= count - 1 else 0
    given, rest = [largest] + [least] * (count - 1), total - largest - least * (count - 1)
    while rest > 0:
        free = [i for i in range(1, count) if given[i] < largest] or [i for i in range(1, count) if given[i] < bound]
        pool, remaining = sum([loads[i] for i in free]), rest
        for i in free:
            addition = min(bound - given[i], max(1, remaining * loads[i] // pool), rest)
            given[i] = given[i] + addition
            rest = rest - addition
    return np.array(given)


def bell_draw(own_key, extent, spread, most, shards=(), held_as=jnp.bfloat16):
    drawn = jax.random.normal(own_key, extent, jnp.float32) * spread
    if len(shards) > 0:
        drawn = shard_levels(own_key, extent, shards, -0.22, 0.18) * drawn
    return jnp.clip(drawn, min=-most, max=most).astype(held_as)


def setup_inputs(seed: int = 0) -> dict:
    arg_keys = jax.random.split(jax.random.key(seed), 5)
    fields = bell_draw(arg_keys[0], (ELEMENTS, ROW), 1.0, 6.0, ((0, 128),))
    coordinates = jnp.clip(jax.random.uniform(arg_keys[1], (3, PROBES), jnp.float32, -1.0, 1.0) * shard_levels(arg_keys[1], (3, PROBES), ((1, 128),), -0.4, 0.0), -1.0, 1.0)
    element_rank_keys = jax.random.split(jax.random.fold_in(arg_keys[2], 1), PROBES // P_DEV)
    element_rank_turns = jax.random.permutation(jax.random.fold_in(arg_keys[2], 3), PROBES // P_DEV)
    element_rank = jax.vmap(lambda own, number: routed_block(jax.random.fold_in(arg_keys[2], 2), own, number, P_DEV, DEVICES, 1, CAP, 2))(element_rank_keys, element_rank_turns).reshape((PROBES, 1))
    element_slot = place_ends(jax.random.randint(arg_keys[3], (PROBES,), 0, E_DEV), jax.random.fold_in(arg_keys[3], 1), 0, E_DEV - 1).astype(jnp.int32)
    return {"fields": fields, "coordinates": coordinates, "element_rank": element_rank, "element_slot": element_slot}


gll_points = np.array([-1.0, -0.8717401485096066, -0.5917001814331423, -0.2092992179024789, 0.2092992179024789, 0.5917001814331423, 0.8717401485096066, 1.0])
gll_scale = np.array([1.0 / np.prod([gll_points[a] - gll_points[b] for b in range(8) if b != a]) for a in range(8)])


def lagrange(coord):
    offsets = coord[None, :] - jnp.asarray(gll_points, coord.dtype)[:, None]
    weights = []
    for node_a in range(8):
        factor = jnp.ones_like(coord) * gll_scale[node_a]
        for node_b in range(8):
            if node_b != node_a:
                factor = factor * offsets[node_b]
        weights.append(factor)
    return jnp.stack(weights, axis=0)


def interpolate(coordinates, element, fields):
    total_rows = element.shape[0]
    block_rows = math.gcd(total_rows, 8192)
    block_count = total_rows // block_rows

    def one_block(pieces):
        coords_block, slots_block = pieces
        weight_r = lagrange(coords_block[0])
        weight_s = lagrange(coords_block[1])
        weight_t = lagrange(coords_block[2]).astype(jnp.bfloat16)
        gathered = jnp.take(fields, slots_block, axis=0).reshape(block_rows, 256, 8)
        along_t = jnp.einsum("nak,kn->na", gathered.astype(jnp.float32), weight_t.astype(jnp.float32), precision=lax.Precision.HIGHEST)
        along_t = along_t.reshape(block_rows, 4, 8, 8)
        along_s = jnp.einsum("nfij,jn->nfi", along_t, weight_s, precision=lax.Precision.HIGHEST)
        return jnp.einsum("nfi,in->fn", along_s, weight_r, precision=lax.Precision.HIGHEST)

    coords_blocks = coordinates.reshape(3, block_count, block_rows).transpose(1, 0, 2)
    slot_blocks = element.reshape(block_count, block_rows)
    result = lax.map(one_block, (coords_blocks, slot_blocks))
    return result.transpose(1, 0, 2).reshape(4, total_rows)


def reference(fields, coordinates, element_rank, element_slot):
    element = element_rank[:, 0].astype(jnp.int32) * E_DEV + element_slot.astype(jnp.int32)
    return interpolate(coordinates, element, fields)
```

```python
import functools

import jax
import jax.numpy as jnp
import numpy as np
from jax import lax
from jax.experimental import pallas as pl
from jax.experimental.pallas import tpu as pltpu
from jax.sharding import PartitionSpec as P

AXES = ("gx", "gy", "gz")
F32, BF16 = jnp.float32, jnp.bfloat16
LANES = 128
CHUNK = 256
PIECE = 32
BLOCKS = 5
PLACED = 8
GATHERED = 4

gll_points = np.array(
    [
        -1.0,
        -0.8717401485096066,
        -0.5917001814331423,
        -0.2092992179024789,
        0.2092992179024789,
        0.5917001814331423,
        0.8717401485096066,
        1.0,
    ]
)
gll_scale = np.array(
    [1.0 / np.prod([gll_points[a] - gll_points[b] for b in range(8) if b != a]) for a in range(8)]
)
node_table = np.stack(
    [gll_scale] + [np.roll(gll_points, -k) for k in range(1, 8)], axis=0
).reshape(64, 1)

RING = [0, 1, 2, 1]


def far_to_near(sizes):
    def hops(q):
        x, y, z = q // (sizes[1] * sizes[2]), (q // sizes[2]) % sizes[1], q % sizes[2]
        return RING[x] + RING[y] + RING[z // 2]

    return sorted(range(sizes[0] * sizes[1] * sizes[2]), key=lambda q: (-hops(q), -q))


def flipped(place, mask):
    return [place, place + 1 - 2 * (place % 2), (place + 2) % 4, 3 - place][mask]


def iota_bf16(shape):
    return lax.broadcasted_iota(jnp.int32, shape, 0).astype(F32).astype(BF16)


def spread(row, count):
    return jnp.broadcast_to(row, (count, row.shape[1])).astype(BF16)


def one_hot(ids, row):
    return jnp.where(ids == spread(row, ids.shape[0]), jnp.ones((), BF16), jnp.zeros((), BF16))


def twice(ids):
    return jnp.concatenate([ids, ids], axis=1)


def chunk_at(step, g, group):
    return pl.ds(pl.multiple_of((step * group + g) * CHUNK, CHUNK), CHUNK)


def place(count, rank_ref, prefix_ref, ids_ref, block_ref, lane_ref):
    probes = rank_ref.shape[1]
    ids = twice(ids_ref[...])

    def body(step, carry):
        hots = [one_hot(ids, rank_ref[:, chunk_at(step, g, PLACED)].astype(F32)) for g in range(PLACED)]
        counted = jnp.dot(jnp.concatenate(hots, axis=0), prefix_ref[...], preferred_element_type=F32)
        for g in range(PLACED):
            at = chunk_at(step, g, PLACED)
            piece = counted[g * count : (g + 1) * count].astype(BF16)
            inside = piece[:, :CHUNK] + twice(carry)
            inside = jnp.where(hots[g] > jnp.zeros((), BF16), inside, jnp.zeros((), BF16))
            total = inside[:16]
            for k in range(1, count // 16):
                total = total + inside[16 * k : 16 * k + 16]
            position = jnp.sum(total.astype(F32), axis=0, keepdims=True) - 1.0
            block = jnp.floor(position * (1.0 / PIECE))
            lane_ref[:, at] = position - block * PIECE
            block_ref[:, at] = block
            carry = carry + piece[:, CHUNK:]
        return carry

    lax.fori_loop(0, probes // (CHUNK * PLACED), body, jnp.zeros((count, LANES), BF16))


def scatter(first, many, rank_ref, coords_ref, slot_ref, block_ref, lane_ref, ids_ref, send_ref, acc_ref):
    probes = rank_ref.shape[1]
    ids = twice(ids_ref[first : first + many, :])
    lane_ids = iota_bf16((PIECE, CHUNK))
    zero = jnp.zeros((), BF16)
    acc_ref[...] = jnp.zeros_like(acc_ref)

    def body(step, _):
        row_hots, lane_parts = [], []
        for g in range(GATHERED):
            at = chunk_at(step, g, GATHERED)
            rank, block, lane = rank_ref[:, at].astype(F32), block_ref[:, at], lane_ref[:, at]
            row_hots.append(
                jnp.concatenate(
                    [one_hot(ids, jnp.where(block == float(b), rank, -1.0)) for b in range(BLOCKS)], axis=0
                )
            )
            here = lane_ids == spread(lane, PIECE)
            high, low = [], []
            for v in range(3):
                value = coords_ref[v : v + 1, at]
                top = value.astype(BF16).astype(F32)
                high.append(top)
                low.append(value - top)
            high.append(slot_ref[:, at].astype(F32))
            chosen = [jnp.where(here, spread(part, PIECE), zero) for part in high + low]
            chosen.append(jnp.zeros((PIECE, CHUNK), BF16))
            lane_parts.append(jnp.concatenate(chosen, axis=0))
        acc_ref[...] += lax.dot_general(
            jnp.concatenate(row_hots, axis=1),
            jnp.concatenate(lane_parts, axis=1),
            (((1,), (1,)), ((), ())),
            preferred_element_type=F32,
        )
        return 0

    lax.fori_loop(0, probes // (GATHERED * CHUNK), body, 0)
    for b in range(BLOCKS):
        rows = slice(b * many, (b + 1) * many)
        send_ref[b, first : first + many, :] = acc_ref[rows, :LANES] + acc_ref[rows, LANES:]


def swap_groups(rows):
    lane = lax.broadcasted_iota(jnp.int32, (8, LANES), 1)
    for width in (2, 1):
        shift = width * PIECE
        lower = (lane // shift) % 2 == 0
        swapped = list(rows)
        for k in range(4):
            if (k // width) % 2 == 0:
                a, b = rows[k], rows[k + width]
                swapped[k] = jnp.where(lower, a, pltpu.roll(b, shift, 1))
                swapped[k + width] = jnp.where(lower, pltpu.roll(a, LANES - shift, 1), b)
        rows = swapped
    return rows


def lagrange(coord, nodes_ref):
    weight = nodes_ref[0:8, :]
    spread_coord = jnp.broadcast_to(coord, (8, LANES))
    for k in range(1, 8):
        weight = weight * (spread_coord - nodes_ref[8 * k : 8 * k + 8, :])
    return weight


def interpolate(rows, fields_ref, nodes_ref, pickers):
    depth = fields_ref.shape[1]
    elements = depth // 8
    zero = jnp.zeros((), BF16)
    ids = iota_bf16((16, LANES))
    pieces = [[] for _ in range(4)]
    for pair in range(len(rows[0]) // 2):
        picker_ref = pickers[pair % len(pickers)]
        weights = []
        for j in range(2):
            r, s, t, slot = [row[2 * pair + j : 2 * pair + j + 1, :] for row in rows]
            weights.append((lagrange(r, nodes_ref), lagrange(s, nodes_ref)))
            weight_t = lagrange(t, nodes_ref)
            columns = slice(j * LANES, (j + 1) * LANES)
            masks = [ids == spread(slot - float(16 * k), 16) for k in range(elements // 16)]
            for c in range(8):
                weight = spread(weight_t[c : c + 1, :], 16)
                for k in range(elements // 16):
                    at = c * elements + k * 16
                    picker_ref[at : at + 16, columns] = jnp.where(masks[k], weight, zero)
        along = jnp.dot(fields_ref[...], picker_ref[...], preferred_element_type=F32)
        for j in range(2):
            weight_r, weight_s = weights[j]
            columns = slice(j * LANES, (j + 1) * LANES)
            factors = [jnp.broadcast_to(weight_r[a : a + 1, :], (8, LANES)) for a in range(8)]
            for f in range(4):
                total = along[f * 64 : f * 64 + 8, columns] * factors[0]
                for a in range(1, 8):
                    total += along[f * 64 + a * 8 : f * 64 + a * 8 + 8, columns] * factors[a]
                pieces[f].append(jnp.sum(total * weight_s, axis=0, keepdims=True))
    return [jnp.concatenate(piece, axis=0) for piece in pieces]


def sample_kernel(
    sizes,
    rank_ref,
    coords_ref,
    slot_ref,
    prefix_ref,
    order_ref,
    fields_ref,
    nodes_ref,
    back_ref,
    block_ref,
    lane_ref,
    ids_ref,
    acc_ref,
    send_ref,
    recv_ref,
    values_ref,
    picker_a,
    picker_b,
    out_sem,
    in_sem,
    back_out_sem,
    back_in_sem,
):
    count = sizes[0] * sizes[1] * sizes[2]
    last = count - 1
    gx, gy, gz = [lax.axis_index(axis) for axis in AXES]
    me = (gx * sizes[1] + gy) * sizes[2] + gz
    order = far_to_near(sizes)
    xs, ys, zs = [[flipped(place, m) for m in range(4)] for place in (gx, gy, gz // 2)]
    cores = [gz % 2, 1 - gz % 2]
    mesh_ids = pl.DeviceIdType.MESH

    def peer(i):
        q = order[i]
        z = q % sizes[2]
        return (xs[q // (sizes[1] * sizes[2])], ys[(q // sizes[2]) % sizes[1]], zs[z // 2] * 2 + cores[z % 2])

    def remote(source, target, sent, arrived, i, device):
        return pltpu.make_async_remote_copy(
            src_ref=source.at[:, i],
            dst_ref=target.at[:, i],
            send_sem=sent.at[i],
            recv_sem=arrived.at[i],
            device_id=device,
            device_id_type=mesh_ids,
        )

    def outward(i, device):
        return remote(send_ref, recv_ref, out_sem, in_sem, i, device)

    def backward(i, device):
        return remote(values_ref, back_ref, back_out_sem, back_in_sem, i, device)

    here = (gx, gy, gz)
    barrier = pltpu.get_barrier_semaphore()
    for i in range(last):
        pl.semaphore_signal(barrier, inc=1, device_id=peer(i), device_id_type=mesh_ids)
    ids_ref[...] = jnp.bitwise_xor(order_ref[...], me).astype(F32).astype(BF16)
    place(count, rank_ref, prefix_ref, ids_ref, block_ref, lane_ref)
    half = count // 2
    for part in range(2):
        scatter(
            part * half, half, rank_ref, coords_ref, slot_ref, block_ref, lane_ref, ids_ref, send_ref, acc_ref
        )
        if part == 0:
            pl.semaphore_wait(barrier, last)
        for i in range(part * half, min((part + 1) * half, last)):
            outward(i, peer(i)).start()
    for b in range(BLOCKS):
        recv_ref[b, last : last + 1, :] = send_ref[b, last : last + 1, :]

    def body(step, _):
        quad, turn = step // 5, step % 5
        tail = turn // 4
        octet = quad * 4 + turn
        base = (1 - tail) * (octet * 8) + tail * (quad * 32)
        for j in range(8):

            @pl.when((1 - tail) * (octet * 8 + j) + tail * last < last)
            def _():
                outward(octet * 8 + j, here).wait_recv()

        spots = []
        for m in range(4):
            row = pl.multiple_of(base + tail * (8 * m), 8)
            spots.append((m * (1 - tail) + 4 * tail, pl.ds(row, 8)))
        rows = swap_groups([recv_ref[b, at, :] for b, at in spots])
        values = swap_groups(interpolate(rows, fields_ref, nodes_ref, [picker_a, picker_b]))
        for (b, at), value in zip(spots, values):
            values_ref[b, at, :] = value

        for g in range(count // 32):

            @pl.when(step == 5 * g + 4)
            def _():
                for i in range(32 * g, min(32 * g + 32, last)):
                    backward(i, peer(i)).start()

        return 0

    lax.fori_loop(0, count // 32 * 5, body, 0)
    for b in range(BLOCKS):
        back_ref[b, last : last + 1, :] = values_ref[b, last : last + 1, :]

    def finish(i, _):
        outward(i, here).wait_send()
        backward(i, here).wait()
        return 0

    lax.fori_loop(0, last, finish, 0)


def return_kernel(values_ref, rank_ref, block_ref, lane_ref, ids_ref, out_ref, table_ref):
    probes = rank_ref.shape[1]
    count = values_ref.shape[1]
    for b in range(BLOCKS):
        table_ref[:, b * count : (b + 1) * count] = values_ref[b].T.astype(BF16)
    ids = twice(ids_ref[...])
    lane_ids = lax.broadcasted_iota(jnp.int32, (PIECE, CHUNK), 0).astype(F32)

    def body(step, _):
        for g in range(4):
            at = chunk_at(step, g, 4)
            rank, block = rank_ref[:, at].astype(F32), block_ref[:, at]
            hot = jnp.concatenate(
                [one_hot(ids, jnp.where(block == float(b), rank, -1.0)) for b in range(BLOCKS)], axis=0
            )
            picked = jnp.dot(table_ref[...], hot, preferred_element_type=F32)
            here = lane_ids == jnp.broadcast_to(lane_ref[:, at], (PIECE, CHUNK))
            for f in range(4):
                out_ref[f : f + 1, at] = jnp.sum(
                    jnp.where(here, picked[f * PIECE : (f + 1) * PIECE], 0.0), axis=0, keepdims=True
                )
        return 0

    lax.fori_loop(0, probes // (4 * CHUNK), body, 0)


VMEM = pl.BlockSpec(memory_space=pltpu.VMEM)


def call(kernel, inputs, outputs, scratch, **options):
    return pl.pallas_call(
        kernel,
        out_shape=outputs,
        in_specs=[VMEM] * inputs,
        out_specs=jax.tree.map(lambda _: VMEM, outputs),
        scratch_shapes=scratch,
        compiler_params=pltpu.CompilerParams(vmem_limit_bytes=48 << 20, **options),
    )


def local(sizes, fields, coordinates, element_rank, element_slot):
    count = sizes[0] * sizes[1] * sizes[2]
    probes = element_slot.shape[0]
    elements = fields.shape[0]
    layout = jax.ShapeDtypeStruct((BLOCKS, count, LANES), F32)
    line = jax.ShapeDtypeStruct((1, probes), F32)

    lower = np.arange(CHUNK)
    prefix = np.concatenate([lower[:, None] <= lower[None, :], np.ones((CHUNK, LANES))], axis=1)
    order = np.broadcast_to(np.array(far_to_near(sizes), np.int32)[:, None], (count, LANES))
    turned = fields.reshape(elements, 256, 8).transpose(1, 2, 0).reshape(256, 8 * elements)
    nodes = jnp.broadcast_to(jnp.asarray(node_table, F32), (64, LANES))
    picker = pltpu.VMEM((8 * elements, 2 * LANES), BF16)
    buffer = pltpu.VMEM(layout.shape, F32)
    arrivals = pltpu.SemaphoreType.DMA((count,))
    rank = element_rank.reshape(1, probes)
    returned, block, lane, ids = call(
        functools.partial(sample_kernel, sizes),
        7,
        (layout, line, line, jax.ShapeDtypeStruct((count, LANES), BF16)),
        [pltpu.VMEM((BLOCKS * count // 2, 2 * LANES), F32)] + [buffer] * 3 + [picker] * 2 + [arrivals] * 4,
        collective_id=0,
        has_side_effects=True,
    )(
        rank,
        coordinates,
        element_slot.reshape(1, probes),
        jnp.asarray(prefix, BF16),
        jnp.asarray(order),
        turned,
        nodes,
    )
    return call(
        return_kernel,
        5,
        jax.ShapeDtypeStruct((4, probes), F32),
        [pltpu.VMEM((LANES, count * BLOCKS), BF16)],
    )(returned, rank, block, lane, ids)


def solution(mesh):
    sizes = tuple(mesh.shape[axis] for axis in AXES)
    placed = (P(AXES, None), P(None, AXES), P(AXES, None), P(AXES))
    return jax.shard_map(
        functools.partial(local, sizes),
        mesh=mesh,
        in_specs=placed,
        out_specs=P(None, AXES),
        check_vma=False,
    )
```

```python
import functools

import jax
import jax.numpy as jnp
import numpy as np
from jax import lax
from jax.experimental import pallas as pl
from jax.experimental.pallas import tpu as pltpu
from jax.sharding import PartitionSpec as P

AXES = ("gx", "gy", "gz")
F32, BF16 = jnp.float32, jnp.bfloat16
LANES = 128
CHUNK = 256
PIECE = 32
BLOCKS = 5
PLACED = 16
GATHERED = 16
RETURNED = 16

gll_points = np.array(
    [
        -1.0,
        -0.8717401485096066,
        -0.5917001814331423,
        -0.2092992179024789,
        0.2092992179024789,
        0.5917001814331423,
        0.8717401485096066,
        1.0,
    ]
)
gll_scale = np.array(
    [1.0 / np.prod([gll_points[a] - gll_points[b] for b in range(8) if b != a]) for a in range(8)]
)
node_table = np.stack(
    [gll_scale] + [np.roll(gll_points, -k) for k in range(1, 8)], axis=0
).reshape(64, 1)

RING = [0, 1, 2, 1]


def far_to_near(sizes):
    def hops(q):
        x, y, z = q // (sizes[1] * sizes[2]), (q // sizes[2]) % sizes[1], q % sizes[2]
        return RING[x] + RING[y] + RING[z // 2]

    return sorted(range(sizes[0] * sizes[1] * sizes[2]), key=lambda q: (-hops(q), -q))


def flipped(place, mask):
    return [place, place + 1 - 2 * (place % 2), (place + 2) % 4, 3 - place][mask]


def iota_bf16(shape):
    return lax.broadcasted_iota(jnp.int32, shape, 0).astype(F32).astype(BF16)


def spread(row, count):
    return jnp.broadcast_to(row, (count, row.shape[1])).astype(BF16)


def one_hot(ids, row):
    return jnp.where(ids == spread(row, ids.shape[0]), jnp.ones((), BF16), jnp.zeros((), BF16))


def twice(ids):
    return jnp.concatenate([ids, ids], axis=1)


def chunk_at(step, g, group):
    return pl.ds(pl.multiple_of((step * group + g) * CHUNK, CHUNK), CHUNK)


def place(count, rank_ref, prefix_ref, ids_ref, block_ref, lane_ref):
    probes = rank_ref.shape[1]
    ids = twice(ids_ref[...])

    def body(step, carry):
        hots = [one_hot(ids, rank_ref[:, chunk_at(step, g, PLACED)].astype(F32)) for g in range(PLACED)]
        counted = jnp.dot(jnp.concatenate(hots, axis=0), prefix_ref[...], preferred_element_type=F32)
        for g in range(PLACED):
            at = chunk_at(step, g, PLACED)
            piece = counted[g * count : (g + 1) * count].astype(BF16)
            inside = piece[:, :CHUNK] + twice(carry)
            inside = jnp.where(hots[g] > jnp.zeros((), BF16), inside, jnp.zeros((), BF16))
            total = inside[:16]
            for k in range(1, count // 16):
                total = total + inside[16 * k : 16 * k + 16]
            position = jnp.sum(total.astype(F32), axis=0, keepdims=True) - 1.0
            block = jnp.floor(position * (1.0 / PIECE))
            lane_ref[:, at] = position - block * PIECE
            block_ref[:, at] = block
            carry = carry + piece[:, CHUNK:]
        return carry

    lax.fori_loop(0, probes // (CHUNK * PLACED), body, jnp.zeros((count, LANES), BF16))


def scatter(first, many, rank_ref, coords_ref, slot_ref, block_ref, lane_ref, ids_ref, send_ref, acc_ref):
    probes = rank_ref.shape[1]
    ids = twice(ids_ref[first : first + many, :])
    lane_ids = iota_bf16((PIECE, CHUNK))
    zero = jnp.zeros((), BF16)
    acc_ref[...] = jnp.zeros_like(acc_ref)

    def body(step, _):
        row_hots, lane_parts = [], []
        for g in range(GATHERED):
            at = chunk_at(step, g, GATHERED)
            rank, block, lane = rank_ref[:, at].astype(F32), block_ref[:, at], lane_ref[:, at]
            row_hots.append(
                jnp.concatenate(
                    [one_hot(ids, jnp.where(block == float(b), rank, -1.0)) for b in range(BLOCKS)], axis=0
                )
            )
            here = lane_ids == spread(lane, PIECE)
            high, low = [], []
            for v in range(3):
                value = coords_ref[v : v + 1, at]
                top = value.astype(BF16).astype(F32)
                high.append(top)
                low.append(value - top)
            high.append(slot_ref[:, at].astype(F32))
            chosen = [jnp.where(here, spread(part, PIECE), zero) for part in high + low]
            chosen.append(jnp.zeros((PIECE, CHUNK), BF16))
            lane_parts.append(jnp.concatenate(chosen, axis=0))
        acc_ref[...] += lax.dot_general(
            jnp.concatenate(row_hots, axis=1),
            jnp.concatenate(lane_parts, axis=1),
            (((1,), (1,)), ((), ())),
            preferred_element_type=F32,
        )
        return 0

    lax.fori_loop(0, probes // (GATHERED * CHUNK), body, 0)
    for b in range(BLOCKS):
        rows = slice(b * many, (b + 1) * many)
        send_ref[b, first : first + many, :] = acc_ref[rows, :LANES] + acc_ref[rows, LANES:]


def swap_groups(rows):
    lane = lax.broadcasted_iota(jnp.int32, (8, LANES), 1)
    for width in (2, 1):
        shift = width * PIECE
        lower = (lane // shift) % 2 == 0
        swapped = list(rows)
        for k in range(4):
            if (k // width) % 2 == 0:
                a, b = rows[k], rows[k + width]
                swapped[k] = jnp.where(lower, a, pltpu.roll(b, shift, 1))
                swapped[k + width] = jnp.where(lower, pltpu.roll(a, LANES - shift, 1), b)
        rows = swapped
    return rows


def lagrange(coord, nodes_ref):
    weight = nodes_ref[0:8, :]
    spread_coord = jnp.broadcast_to(coord, (8, LANES))
    for k in range(1, 8):
        weight = weight * (spread_coord - nodes_ref[8 * k : 8 * k + 8, :])
    return weight


def interpolate(rows, fields_ref, nodes_ref):
    depth = fields_ref.shape[1]
    elements = depth // 8
    zero = jnp.zeros((), BF16)
    ids = iota_bf16((16, LANES))
    pieces = [[] for _ in range(4)]
    for pair in range(len(rows[0]) // 2):
        weights, columns_of = [], []
        for j in range(2):
            r, s, t, slot = [row[2 * pair + j : 2 * pair + j + 1, :] for row in rows]
            weights.append((lagrange(r, nodes_ref), lagrange(s, nodes_ref)))
            weight_t = lagrange(t, nodes_ref)
            spread_t = [spread(weight_t[c : c + 1, :], 16) for c in range(8)]
            hots = [
                jnp.where(ids == spread(slot - float(16 * k), 16), jnp.ones((), BF16), zero)
                for k in range(elements // 16)
            ]
            columns_of.append(jnp.concatenate([hot * weight for weight in spread_t for hot in hots], axis=0))
        picker = jnp.concatenate(columns_of, axis=1)
        along = jnp.dot(fields_ref[...], picker, preferred_element_type=F32)
        for j in range(2):
            weight_r, weight_s = weights[j]
            columns = slice(j * LANES, (j + 1) * LANES)
            factors = [jnp.broadcast_to(weight_r[a : a + 1, :], (8, LANES)) for a in range(8)]
            for f in range(4):
                total = along[f * 64 : f * 64 + 8, columns] * factors[0]
                for a in range(1, 8):
                    total += along[f * 64 + a * 8 : f * 64 + a * 8 + 8, columns] * factors[a]
                pieces[f].append(jnp.sum(total * weight_s, axis=0, keepdims=True))
    return [jnp.concatenate(piece, axis=0) for piece in pieces]


def sample_kernel(
    sizes,
    rank_ref,
    coords_ref,
    slot_ref,
    prefix_ref,
    order_ref,
    fields_ref,
    nodes_ref,
    back_ref,
    block_ref,
    lane_ref,
    ids_ref,
    acc_ref,
    send_ref,
    recv_ref,
    values_ref,
    out_sem,
    in_sem,
    back_out_sem,
    back_in_sem,
):
    count = sizes[0] * sizes[1] * sizes[2]
    last = count - 1
    gx, gy, gz = [lax.axis_index(axis) for axis in AXES]
    me = (gx * sizes[1] + gy) * sizes[2] + gz
    order = far_to_near(sizes)
    xs, ys, zs = [[flipped(place, m) for m in range(4)] for place in (gx, gy, gz // 2)]
    cores = [gz % 2, 1 - gz % 2]
    mesh_ids = pl.DeviceIdType.MESH

    def peer(i):
        q = order[i]
        z = q % sizes[2]
        return (xs[q // (sizes[1] * sizes[2])], ys[(q // sizes[2]) % sizes[1]], zs[z // 2] * 2 + cores[z % 2])

    def remote(source, target, sent, arrived, i, device):
        return pltpu.make_async_remote_copy(
            src_ref=source.at[:, i],
            dst_ref=target.at[:, i],
            send_sem=sent.at[i],
            recv_sem=arrived.at[i],
            device_id=device,
            device_id_type=mesh_ids,
        )

    def outward(i, device):
        return remote(send_ref, recv_ref, out_sem, in_sem, i, device)

    def backward(i, device):
        return remote(values_ref, back_ref, back_out_sem, back_in_sem, i, device)

    here = (gx, gy, gz)
    barrier = pltpu.get_barrier_semaphore()
    for i in range(last):
        pl.semaphore_signal(barrier, inc=1, device_id=peer(i), device_id_type=mesh_ids)
    ids_ref[...] = jnp.bitwise_xor(order_ref[...], me).astype(F32).astype(BF16)
    place(count, rank_ref, prefix_ref, ids_ref, block_ref, lane_ref)
    half = count // 2
    for part in range(2):
        scatter(
            part * half, half, rank_ref, coords_ref, slot_ref, block_ref, lane_ref, ids_ref, send_ref, acc_ref
        )
        if part == 0:
            pl.semaphore_wait(barrier, last)
        for i in range(part * half, min((part + 1) * half, last)):
            outward(i, peer(i)).start()
    for b in range(BLOCKS):
        recv_ref[b, last : last + 1, :] = send_ref[b, last : last + 1, :]

    def body(quad, _):
        for j in range(32):

            @pl.when(quad * 32 + j < last)
            def _():
                outward(quad * 32 + j, here).wait_recv()

        for turn in range(5):
            spots = []
            for m in range(4):
                row = pl.multiple_of(quad * 32 + 8 * (turn if turn < 4 else m), 8)
                spots.append((m if turn < 4 else 4, pl.ds(row, 8)))
            rows = swap_groups([recv_ref[b, at, :] for b, at in spots])
            values = swap_groups(interpolate(rows, fields_ref, nodes_ref))
            for (b, at), value in zip(spots, values):
                values_ref[b, at, :] = value

        for g in range(count // 32):

            @pl.when(quad == g)
            def _():
                for i in range(32 * g, min(32 * g + 32, last)):
                    backward(i, peer(i)).start()

        return 0

    lax.fori_loop(0, count // 32, body, 0)
    for b in range(BLOCKS):
        back_ref[b, last : last + 1, :] = values_ref[b, last : last + 1, :]

    def finish(i, _):
        outward(i, here).wait_send()
        backward(i, here).wait()
        return 0

    lax.fori_loop(0, last, finish, 0)


def return_kernel(values_ref, rank_ref, block_ref, lane_ref, ids_ref, out_ref, table_ref):
    probes = rank_ref.shape[1]
    count = values_ref.shape[1]
    for b in range(BLOCKS):
        table_ref[:, b * count : (b + 1) * count] = values_ref[b].T.astype(BF16)
    ids = twice(ids_ref[...])
    lane_ids = lax.broadcasted_iota(jnp.int32, (PIECE, CHUNK), 0).astype(F32)

    def body(step, _):
        for g in range(RETURNED):
            at = chunk_at(step, g, RETURNED)
            rank, block = rank_ref[:, at].astype(F32), block_ref[:, at]
            hot = jnp.concatenate(
                [one_hot(ids, jnp.where(block == float(b), rank, -1.0)) for b in range(BLOCKS)], axis=0
            )
            picked = jnp.dot(table_ref[...], hot, preferred_element_type=F32)
            here = lane_ids == jnp.broadcast_to(lane_ref[:, at], (PIECE, CHUNK))
            for f in range(4):
                out_ref[f : f + 1, at] = jnp.sum(
                    jnp.where(here, picked[f * PIECE : (f + 1) * PIECE], 0.0), axis=0, keepdims=True
                )
        return 0

    lax.fori_loop(0, probes // (RETURNED * CHUNK), body, 0)


VMEM = pl.BlockSpec(memory_space=pltpu.VMEM)


def call(kernel, inputs, outputs, scratch, **options):
    return pl.pallas_call(
        kernel,
        out_shape=outputs,
        in_specs=[VMEM] * inputs,
        out_specs=jax.tree.map(lambda _: VMEM, outputs),
        scratch_shapes=scratch,
        compiler_params=pltpu.CompilerParams(vmem_limit_bytes=48 << 20, **options),
    )


def local(sizes, fields, coordinates, element_rank, element_slot):
    count = sizes[0] * sizes[1] * sizes[2]
    probes = element_slot.shape[0]
    elements = fields.shape[0]
    layout = jax.ShapeDtypeStruct((BLOCKS, count, LANES), F32)
    line = jax.ShapeDtypeStruct((1, probes), F32)

    lower = np.arange(CHUNK)
    prefix = np.concatenate([lower[:, None] <= lower[None, :], np.ones((CHUNK, LANES))], axis=1)
    order = np.broadcast_to(np.array(far_to_near(sizes), np.int32)[:, None], (count, LANES))
    turned = fields.reshape(elements, 256, 8).transpose(1, 2, 0).reshape(256, 8 * elements)
    nodes = jnp.broadcast_to(jnp.asarray(node_table, F32), (64, LANES))
    buffer = pltpu.VMEM(layout.shape, F32)
    arrivals = pltpu.SemaphoreType.DMA((count,))
    rank = element_rank.reshape(1, probes)
    returned, block, lane, ids = call(
        functools.partial(sample_kernel, sizes),
        7,
        (layout, line, line, jax.ShapeDtypeStruct((count, LANES), BF16)),
        [pltpu.VMEM((BLOCKS * count // 2, 2 * LANES), F32)] + [buffer] * 3 + [arrivals] * 4,
        collective_id=0,
        has_side_effects=True,
    )(
        rank,
        coordinates,
        element_slot.reshape(1, probes),
        jnp.asarray(prefix, BF16),
        jnp.asarray(order),
        turned,
        nodes,
    )
    return call(
        return_kernel,
        5,
        jax.ShapeDtypeStruct((4, probes), F32),
        [pltpu.VMEM((LANES, count * BLOCKS), BF16)],
    )(returned, rank, block, lane, ids)


def solution(mesh):
    sizes = tuple(mesh.shape[axis] for axis in AXES)
    placed = (P(AXES, None), P(None, AXES), P(AXES, None), P(AXES))
    return jax.shard_map(
        functools.partial(local, sizes),
        mesh=mesh,
        in_specs=placed,
        out_specs=P(None, AXES),
        check_vma=False,
    )
```

```python
import functools

import jax
import jax.numpy as jnp
import numpy as np
from jax import lax
from jax.experimental import pallas as pl
from jax.experimental.pallas import tpu as pltpu
from jax.sharding import PartitionSpec as P

AXES = ("gx", "gy", "gz")
F32, BF16 = jnp.float32, jnp.bfloat16
LANES = 128
CHUNK = 256
PIECE = 32
BLOCKS = 5
PLACED = 16
GATHERED = 16
RETURNED = 16

gll_points = np.array(
    [
        -1.0,
        -0.8717401485096066,
        -0.5917001814331423,
        -0.2092992179024789,
        0.2092992179024789,
        0.5917001814331423,
        0.8717401485096066,
        1.0,
    ]
)
gll_scale = np.array(
    [1.0 / np.prod([gll_points[a] - gll_points[b] for b in range(8) if b != a]) for a in range(8)]
)
node_table = np.stack([gll_scale] + [np.roll(gll_points, -k) for k in range(1, 8)], axis=0)

RING = [0, 1, 2, 1]


def served(sizes):
    def hops(q):
        x, y, z = q // (sizes[1] * sizes[2]), (q // sizes[2]) % sizes[1], q % sizes[2]
        return RING[x] + RING[y] + RING[z // 2]

    far = sorted(range(sizes[0] * sizes[1] * sizes[2]), key=lambda q: (-hops(q), -q))
    return far[96:] + far[:32] + far[32:96]


def flipped(place, mask):
    return [place, place + 1 - 2 * (place % 2), (place + 2) % 4, 3 - place][mask]


def iota_bf16(shape):
    return lax.broadcasted_iota(jnp.int32, shape, 0).astype(F32).astype(BF16)


def spread(row, count):
    return jnp.broadcast_to(row, (count, row.shape[1])).astype(BF16)


def one_hot(ids, row):
    return jnp.where(ids == spread(row, ids.shape[0]), jnp.ones((), BF16), jnp.zeros((), BF16))


def twice(ids):
    return jnp.concatenate([ids, ids], axis=1)


def chunk_at(step, g, group):
    return pl.ds(pl.multiple_of((step * group + g) * CHUNK, CHUNK), CHUNK)


def place(count, rank_ref, ids_ref, block_ref, lane_ref):
    probes = rank_ref.shape[1]
    ids = twice(ids_ref[...])
    before = lax.broadcasted_iota(jnp.int32, (CHUNK, CHUNK), 0) <= lax.broadcasted_iota(jnp.int32, (CHUNK, CHUNK), 1)
    prefix = jnp.where(before, 1.0, 0.0).astype(BF16)

    def body(step, carry):
        hots = [one_hot(ids, rank_ref[:, chunk_at(step, g, PLACED)].astype(F32)) for g in range(PLACED)]
        counted = jnp.dot(jnp.concatenate(hots, axis=0), prefix, preferred_element_type=F32)
        for g in range(PLACED):
            at = chunk_at(step, g, PLACED)
            piece = counted[g * count : (g + 1) * count].astype(BF16)
            inside = (piece + twice(carry)) * hots[g]
            total = inside[:16]
            for k in range(1, count // 16):
                total = total + inside[16 * k : 16 * k + 16]
            position = jnp.sum(total.astype(F32), axis=0, keepdims=True) - 1.0
            block = jnp.floor(position * (1.0 / PIECE))
            lane_ref[:, at] = position - block * PIECE
            block_ref[:, at] = block
            carry = carry + jnp.broadcast_to(piece[:, CHUNK - 1 :], carry.shape)
        return carry

    lax.fori_loop(0, probes // (CHUNK * PLACED), body, jnp.zeros((count, LANES), BF16))


def scatter(first, many, rank_ref, coords_ref, slot_ref, block_ref, lane_ref, ids_ref, send_ref, acc_ref):
    probes = rank_ref.shape[1]
    ids = twice(ids_ref[first : first + many, :])
    lane_ids = iota_bf16((PIECE, CHUNK))
    zero = jnp.zeros((), BF16)
    acc_ref[...] = jnp.zeros_like(acc_ref)

    def body(step, _):
        row_hots, lane_parts = [], []
        for g in range(GATHERED):
            at = chunk_at(step, g, GATHERED)
            rank, block, lane = rank_ref[:, at].astype(F32), block_ref[:, at], lane_ref[:, at]
            row_hots.append(
                jnp.concatenate(
                    [one_hot(ids, jnp.where(block == float(b), rank, -1.0)) for b in range(BLOCKS)], axis=0
                )
            )
            here = lane_ids == spread(lane, PIECE)
            high, low = [], []
            for v in range(3):
                value = coords_ref[v : v + 1, at]
                top = value.astype(BF16).astype(F32)
                high.append(top)
                low.append(value - top)
            high.append(slot_ref[:, at].astype(F32))
            chosen = [jnp.where(here, spread(part, PIECE), zero) for part in high + low]
            chosen.append(jnp.zeros((PIECE, CHUNK), BF16))
            lane_parts.append(jnp.concatenate(chosen, axis=0))
        acc_ref[...] += lax.dot_general(
            jnp.concatenate(row_hots, axis=1),
            jnp.concatenate(lane_parts, axis=1),
            (((1,), (1,)), ((), ())),
            preferred_element_type=F32,
        )
        return 0

    lax.fori_loop(0, probes // (GATHERED * CHUNK), body, 0)
    for b in range(BLOCKS):
        rows = slice(b * many, (b + 1) * many)
        send_ref[b, first : first + many, :] = acc_ref[rows, :LANES] + acc_ref[rows, LANES:]


def swap_groups(rows):
    lane = lax.broadcasted_iota(jnp.int32, (8, LANES), 1)
    for width in (2, 1):
        shift = width * PIECE
        lower = (lane // shift) % 2 == 0
        swapped = list(rows)
        for k in range(4):
            if (k // width) % 2 == 0:
                a, b = rows[k], rows[k + width]
                swapped[k] = jnp.where(lower, a, pltpu.roll(b, shift, 1))
                swapped[k + width] = jnp.where(lower, pltpu.roll(a, LANES - shift, 1), b)
        rows = swapped
    return rows


def write_nodes(nodes_ref):
    row = lax.broadcasted_iota(jnp.int32, (8, LANES), 0)
    for k in range(8):
        value = jnp.full((8, LANES), float(node_table[k, 0]), F32)
        for a in range(1, 8):
            value = jnp.where(row == a, float(node_table[k, a]), value)
        nodes_ref[8 * k : 8 * k + 8, :] = value


def turn_fields(fields_ref, spaced_ref, turned_ref):
    elements = fields_ref.shape[0]
    for k in range(fields_ref.shape[1] // LANES):
        spaced_ref[k * LANES : (k + 1) * LANES, :] = fields_ref[:, k * LANES : (k + 1) * LANES].astype(F32).T
    for c in range(8):
        turned_ref[:, c * elements : (c + 1) * elements] = spaced_ref[pl.ds(c, 256, stride=8), :].astype(BF16)


def lagrange(coord, nodes_ref):
    weight = nodes_ref[0:8, :]
    spread_coord = jnp.broadcast_to(coord, (8, LANES))
    for k in range(1, 8):
        weight = weight * (spread_coord - nodes_ref[8 * k : 8 * k + 8, :])
    return weight


def interpolate(rows, fields_ref, nodes_ref):
    depth = fields_ref.shape[1]
    elements = depth // 8
    zero = jnp.zeros((), BF16)
    ids = iota_bf16((16, LANES))
    pieces = [[] for _ in range(4)]
    for pair in range(len(rows[0]) // 2):
        weights, columns_of = [], []
        for j in range(2):
            r, s, t, slot = [row[2 * pair + j : 2 * pair + j + 1, :] for row in rows]
            weights.append((lagrange(r, nodes_ref), lagrange(s, nodes_ref)))
            weight_t = lagrange(t, nodes_ref)
            spread_t = [spread(weight_t[c : c + 1, :], 16) for c in range(8)]
            hots = [
                jnp.where(ids == spread(slot - float(16 * k), 16), jnp.ones((), BF16), zero)
                for k in range(elements // 16)
            ]
            columns_of.append(jnp.concatenate([hot * weight for weight in spread_t for hot in hots], axis=0))
        picker = jnp.concatenate(columns_of, axis=1)
        along = jnp.dot(fields_ref[...], picker, preferred_element_type=F32)
        for j in range(2):
            weight_r, weight_s = weights[j]
            columns = slice(j * LANES, (j + 1) * LANES)
            factors = [jnp.broadcast_to(weight_r[a : a + 1, :], (8, LANES)) for a in range(8)]
            for f in range(4):
                total = along[f * 64 : f * 64 + 8, columns] * factors[0]
                for a in range(1, 8):
                    total += along[f * 64 + a * 8 : f * 64 + a * 8 + 8, columns] * factors[a]
                pieces[f].append(jnp.sum(total * weight_s, axis=0, keepdims=True))
    return [jnp.concatenate(piece, axis=0) for piece in pieces]


def sample_kernel(
    sizes,
    rank_hbm,
    coords_hbm,
    slot_hbm,
    fields_hbm,
    part_ref,
    late_ref,
    block_ref,
    lane_ref,
    ids_ref,
    acc_ref,
    spaced_ref,
    turned_ref,
    table_ref,
    nodes_ref,
    rank_ref,
    coords_ref,
    slot_ref,
    fields_ref,
    back_ref,
    send_ref,
    recv_ref,
    values_ref,
    load_sem,
    out_sem,
    in_sem,
    back_out_sem,
    back_in_sem,
):
    count = sizes[0] * sizes[1] * sizes[2]
    order = served(sizes)
    own, quads = order.index(0), count // 32
    gx, gy, gz = [lax.axis_index(axis) for axis in AXES]
    xs, ys, zs = [[flipped(place, m) for m in range(4)] for place in (gx, gy, gz // 2)]
    cores = [gz % 2, 1 - gz % 2]
    mesh_ids = pl.DeviceIdType.MESH

    def peer(i):
        q = order[i]
        z = q % sizes[2]
        return (xs[q // (sizes[1] * sizes[2])], ys[(q // sizes[2]) % sizes[1]], zs[z // 2] * 2 + cores[z % 2])

    def remote(source, target, sent, arrived, i, device):
        return pltpu.make_async_remote_copy(
            src_ref=source.at[:, i],
            dst_ref=target.at[:, i],
            send_sem=sent.at[i],
            recv_sem=arrived.at[i],
            device_id=device,
            device_id_type=mesh_ids,
        )

    def outward(i, device):
        return remote(send_ref, recv_ref, out_sem, in_sem, i, device)

    def backward(i, device):
        return remote(values_ref, back_ref, back_out_sem, back_in_sem, i, device)

    loads = [
        pltpu.make_async_copy(source, target, load_sem.at[k])
        for k, (source, target) in enumerate(
            [(rank_hbm, rank_ref), (coords_hbm, coords_ref), (slot_hbm, slot_ref), (fields_hbm, fields_ref)]
        )
    ]
    for load in loads:
        load.start()
    here = (gx, gy, gz)
    barrier = pltpu.get_barrier_semaphore()
    for i in range(count):
        if i == own:
            continue
        pl.semaphore_signal(barrier, inc=1, device_id=peer(i), device_id_type=mesh_ids)
    for i in range(count):
        x, y, z = peer(i)
        place_of = (x * sizes[1] + y) * sizes[2] + z
        spaced_ref[i : i + 1, :] = jnp.broadcast_to(place_of.astype(F32), (1, LANES))
    ids_ref[...] = spaced_ref[:count, :].astype(BF16)
    write_nodes(nodes_ref)
    loads[0].wait()
    place(count, rank_ref, ids_ref, block_ref, lane_ref)
    loads[1].wait()
    loads[2].wait()
    half = count // 2
    for part in range(2):
        scatter(
            part * half, half, rank_ref, coords_ref, slot_ref, block_ref, lane_ref, ids_ref, send_ref, acc_ref
        )
        if part == 0:
            pl.semaphore_wait(barrier, count - 1)
        for i in range(part * half, (part + 1) * half):
            if i != own:
                outward(i, peer(i)).start()
    for b in range(BLOCKS):
        recv_ref[b, own : own + 1, :] = send_ref[b, own : own + 1, :]
    loads[3].wait()
    turn_fields(fields_ref, spaced_ref, turned_ref)

    def body(quad, _):
        for j in range(32):

            @pl.when(quad * 32 + j != own)
            def _():
                outward(quad * 32 + j, here).wait_recv()

        for turn in range(5):
            spots = []
            for m in range(4):
                row = pl.multiple_of(quad * 32 + 8 * (turn if turn < 4 else m), 8)
                spots.append((m if turn < 4 else 4, pl.ds(row, 8)))
            rows = swap_groups([recv_ref[b, at, :] for b, at in spots])
            values = swap_groups(interpolate(rows, turned_ref, nodes_ref))
            for (b, at), value in zip(spots, values):
                values_ref[b, at, :] = value

        for g in range(quads):

            @pl.when(quad == g)
            def _():
                for i in range(32 * g, 32 * g + 32):
                    if i != own:
                        backward(i, peer(i)).start()

        return 0

    lax.fori_loop(0, quads, body, 0)
    for b in range(BLOCKS):
        back_ref[b, own : own + 1, :] = values_ref[b, own : own + 1, :]

    def finish(i, _):
        @pl.when(i != own)
        def _():
            outward(i, here).wait_send()
            backward(i, here).wait()

        return 0

    early = count - 32
    lax.fori_loop(0, early, finish, 0)
    rows = [back_ref[b, :early, :] for b in range(BLOCKS)]
    rows.append(jnp.zeros((-BLOCKS * early % LANES, LANES), F32))
    table_ref[...] = jnp.concatenate(rows, axis=0).T.astype(BF16)
    pick(table_ref, ids_ref[:early, :], rank_ref, block_ref, lane_ref, None, part_ref)
    lax.fori_loop(early, count, finish, 0)
    for b in range(BLOCKS):
        late_ref[b * 32 : (b + 1) * 32, :] = back_ref[b, early:, :]


def pick(table_ref, ids, rank_ref, block_ref, lane_ref, part_ref, out_ref):
    probes = rank_ref.shape[1]
    ids = twice(ids)
    lane_ids = lax.broadcasted_iota(jnp.int32, (PIECE, CHUNK), 0).astype(F32)

    def body(step, _):
        for g in range(RETURNED):
            at = chunk_at(step, g, RETURNED)
            rank, block = rank_ref[:, at].astype(F32), block_ref[:, at]
            hots = [one_hot(ids, jnp.where(block == float(b), rank, -1.0)) for b in range(BLOCKS)]
            spare = table_ref.shape[1] - BLOCKS * ids.shape[0]
            if spare:
                hots.append(jnp.zeros((spare, CHUNK), BF16))
            picked = jnp.dot(table_ref[...], jnp.concatenate(hots, axis=0), preferred_element_type=F32)
            here = lane_ids == jnp.broadcast_to(lane_ref[:, at], (PIECE, CHUNK))
            for f in range(4):
                value = jnp.sum(
                    jnp.where(here, picked[f * PIECE : (f + 1) * PIECE], 0.0), axis=0, keepdims=True
                )
                out_ref[f : f + 1, at] = value if part_ref is None else value + part_ref[f : f + 1, at]
        return 0

    lax.fori_loop(0, probes // (RETURNED * CHUNK), body, 0)


def return_kernel(late_ref, part_ref, rank_ref, block_ref, lane_ref, ids_ref, out_ref, table_ref):
    late = late_ref.shape[0]
    rows = jnp.concatenate([late_ref[...], jnp.zeros((-late % LANES, LANES), F32)], axis=0)
    table_ref[...] = rows.T.astype(BF16)
    pick(table_ref, ids_ref[-(late // BLOCKS) :, :], rank_ref, block_ref, lane_ref, part_ref, out_ref)


VMEM = pl.BlockSpec(memory_space=pltpu.VMEM)
HBM = pl.BlockSpec(memory_space=pltpu.HBM)


def call(kernel, inputs, outputs, scratch, **options):
    return pl.pallas_call(
        kernel,
        out_shape=outputs,
        in_specs=inputs,
        out_specs=jax.tree.map(lambda _: VMEM, outputs),
        scratch_shapes=scratch,
        compiler_params=pltpu.CompilerParams(vmem_limit_bytes=48 << 20, **options),
    )


def local(sizes, fields, coordinates, element_rank, element_slot):
    count = sizes[0] * sizes[1] * sizes[2]
    probes = element_slot.shape[0]
    elements = fields.shape[0]
    line = jax.ShapeDtypeStruct((1, probes), F32)

    buffer = pltpu.VMEM((BLOCKS, count, LANES), F32)
    arrivals = pltpu.SemaphoreType.DMA((count,))
    rank = element_rank.reshape(1, probes)
    late = BLOCKS * 32
    whole = jax.ShapeDtypeStruct((4, probes), F32)
    part, returned, block, lane, ids = call(
        functools.partial(sample_kernel, sizes),
        [HBM] * 4,
        (
            whole,
            jax.ShapeDtypeStruct((late, LANES), F32),
            line,
            line,
            jax.ShapeDtypeStruct((count, LANES), BF16),
        ),
        [
            pltpu.VMEM((BLOCKS * count // 2, 2 * LANES), F32),
            pltpu.VMEM((256 * 8, elements), F32),
            pltpu.VMEM((256, 8 * elements), BF16),
            pltpu.VMEM((LANES, -(-BLOCKS * (count - 32) // LANES) * LANES), BF16),
        ]
        + [
            pltpu.VMEM((64, LANES), F32),
            pltpu.VMEM(rank.shape, jnp.int32),
            pltpu.VMEM(coordinates.shape, F32),
            pltpu.VMEM(rank.shape, jnp.int32),
            pltpu.VMEM(fields.shape, BF16),
        ]
        + [buffer] * 4
        + [pltpu.SemaphoreType.DMA((4,))]
        + [arrivals] * 4,
        collective_id=0,
        has_side_effects=True,
    )(
        *[
            pltpu.with_memory_space_constraint(array, pltpu.HBM)
            for array in (rank, coordinates, element_slot.reshape(1, probes), fields)
        ]
    )
    return call(
        return_kernel,
        [VMEM] * 6,
        whole,
        [pltpu.VMEM((LANES, -(-late // LANES) * LANES), BF16)],
    )(returned, part, rank, block, lane, ids)


def solution(mesh):
    sizes = tuple(mesh.shape[axis] for axis in AXES)
    placed = (P(AXES, None), P(None, AXES), P(AXES, None), P(AXES))
    return jax.shard_map(
        functools.partial(local, sizes),
        mesh=mesh,
        in_specs=placed,
        out_specs=P(None, AXES),
        check_vma=False,
    )
```

```python
import functools

import jax
import jax.numpy as jnp
import numpy as np
from jax import lax
from jax.experimental import pallas as pl
from jax.experimental.pallas import tpu as pltpu
from jax.sharding import PartitionSpec as P

AXES = ("gx", "gy", "gz")
F32, BF16 = jnp.float32, jnp.bfloat16
LANES = 128
CHUNK = 256
PIECE = 32
BLOCKS = 5
QUAD = 32
PLACED = 16
GATHERED = 16
RETURNED = 16

gll_points = np.array(
    [
        -1.0,
        -0.8717401485096066,
        -0.5917001814331423,
        -0.2092992179024789,
        0.2092992179024789,
        0.5917001814331423,
        0.8717401485096066,
        1.0,
    ]
)
gll_scale = np.array(
    [1.0 / np.prod([gll_points[a] - gll_points[b] for b in range(8) if b != a]) for a in range(8)]
)
node_table = np.stack([gll_scale] + [np.roll(gll_points, -k) for k in range(1, 8)], axis=0)

REACHED = ((0.0, 1.1, 1.2, 1.6), (0.0, 1.3, 1.5, 1.8), (0.0, 1.5, 2.3, 2.8))


def served(sizes):
    def reached(rank):
        x, y, z = rank // (sizes[1] * sizes[2]), (rank // sizes[2]) % sizes[1], rank % sizes[2] // 2
        return REACHED[0][x] + REACHED[1][y] + REACHED[2][z]

    return sorted(range(sizes[0] * sizes[1] * sizes[2]), key=lambda rank: (reached(rank), rank))


def iota_bf16(shape):
    return lax.broadcasted_iota(jnp.int32, shape, 0).astype(F32).astype(BF16)


def spread(row, count):
    return jnp.broadcast_to(row, (count, row.shape[1])).astype(BF16)


def one_hot(ids, row):
    return jnp.where(ids == spread(row, ids.shape[0]), jnp.ones((), BF16), jnp.zeros((), BF16))


def twice(ids):
    return jnp.concatenate([ids, ids], axis=1)


def chunk_at(step, g, group):
    return pl.ds(pl.multiple_of((step * group + g) * CHUNK, CHUNK), CHUNK)


def place(count, rank_ref, ids_ref, block_ref, lane_ref):
    probes = rank_ref.shape[1]
    ids = twice(ids_ref[...])
    before = lax.broadcasted_iota(jnp.int32, (CHUNK, CHUNK), 0) <= lax.broadcasted_iota(jnp.int32, (CHUNK, CHUNK), 1)
    prefix = jnp.where(before, 1.0, 0.0).astype(BF16)

    def body(step, carry):
        hots = [one_hot(ids, rank_ref[:, chunk_at(step, g, PLACED)].astype(F32)) for g in range(PLACED)]
        counted = jnp.dot(jnp.concatenate(hots, axis=0), prefix, preferred_element_type=F32)
        for g in range(PLACED):
            at = chunk_at(step, g, PLACED)
            piece = counted[g * count : (g + 1) * count].astype(BF16)
            inside = (piece + twice(carry)) * hots[g]
            total = inside[:16]
            for k in range(1, count // 16):
                total = total + inside[16 * k : 16 * k + 16]
            position = jnp.sum(total.astype(F32), axis=0, keepdims=True) - 1.0
            block = jnp.floor(position * (1.0 / PIECE))
            lane_ref[:, at] = position - block * PIECE
            block_ref[:, at] = block
            carry = carry + jnp.broadcast_to(piece[:, CHUNK - 1 :], carry.shape)
        return carry

    lax.fori_loop(0, probes // (CHUNK * PLACED), body, jnp.zeros((count, LANES), BF16))


def scatter(first, many, rank_ref, coords_ref, slot_ref, block_ref, lane_ref, ids_ref, send_ref, acc_ref):
    probes = rank_ref.shape[1]
    ids = twice(ids_ref[first : first + many, :])
    lane_ids = iota_bf16((PIECE, CHUNK))
    zero = jnp.zeros((), BF16)
    acc_ref[...] = jnp.zeros_like(acc_ref)

    def body(step, _):
        row_hots, lane_parts = [], []
        for g in range(GATHERED):
            at = chunk_at(step, g, GATHERED)
            rank, block, lane = rank_ref[:, at].astype(F32), block_ref[:, at], lane_ref[:, at]
            row_hots.append(
                jnp.concatenate(
                    [one_hot(ids, jnp.where(block == float(b), rank, -1.0)) for b in range(BLOCKS)], axis=0
                )
            )
            here = lane_ids == spread(lane, PIECE)
            high, low = [], []
            for v in range(3):
                value = coords_ref[v : v + 1, at]
                top = value.astype(BF16).astype(F32)
                high.append(top)
                low.append(value - top)
            high.append(slot_ref[:, at].astype(F32))
            chosen = [jnp.where(here, spread(part, PIECE), zero) for part in high + low]
            chosen.append(jnp.zeros((PIECE, CHUNK), BF16))
            lane_parts.append(jnp.concatenate(chosen, axis=0))
        acc_ref[...] += lax.dot_general(
            jnp.concatenate(row_hots, axis=1),
            jnp.concatenate(lane_parts, axis=1),
            (((1,), (1,)), ((), ())),
            preferred_element_type=F32,
        )
        return 0

    lax.fori_loop(0, probes // (GATHERED * CHUNK), body, 0)
    for b in range(BLOCKS):
        rows = slice(b * many, (b + 1) * many)
        send_ref[b, first : first + many, :] = acc_ref[rows, :LANES] + acc_ref[rows, LANES:]


def swap_groups(rows):
    lane = lax.broadcasted_iota(jnp.int32, (8, LANES), 1)
    for width in (2, 1):
        shift = width * PIECE
        lower = (lane // shift) % 2 == 0
        swapped = list(rows)
        for k in range(4):
            if (k // width) % 2 == 0:
                a, b = rows[k], rows[k + width]
                swapped[k] = jnp.where(lower, a, pltpu.roll(b, shift, 1))
                swapped[k + width] = jnp.where(lower, pltpu.roll(a, LANES - shift, 1), b)
        rows = swapped
    return rows


def write_nodes(nodes_ref):
    row = lax.broadcasted_iota(jnp.int32, (8, LANES), 0)
    for k in range(8):
        value = jnp.full((8, LANES), float(node_table[k, 0]), F32)
        for a in range(1, 8):
            value = jnp.where(row == a, float(node_table[k, a]), value)
        nodes_ref[8 * k : 8 * k + 8, :] = value


def turn_fields(fields_ref, spaced_ref, turned_ref):
    elements = fields_ref.shape[0]
    for k in range(fields_ref.shape[1] // LANES):
        spaced_ref[k * LANES : (k + 1) * LANES, :] = fields_ref[:, k * LANES : (k + 1) * LANES].astype(F32).T
    for c in range(8):
        turned_ref[:, c * elements : (c + 1) * elements] = spaced_ref[pl.ds(c, 256, stride=8), :].astype(BF16)


def lagrange(coord, nodes_ref):
    weight = nodes_ref[0:8, :]
    spread_coord = jnp.broadcast_to(coord, (8, LANES))
    for k in range(1, 8):
        weight = weight * (spread_coord - nodes_ref[8 * k : 8 * k + 8, :])
    return weight


def interpolate(rows, fields_ref, nodes_ref):
    depth = fields_ref.shape[1]
    elements = depth // 8
    zero = jnp.zeros((), BF16)
    ids = iota_bf16((16, LANES))
    pieces = [[] for _ in range(4)]
    for pair in range(len(rows[0]) // 2):
        weights, columns_of = [], []
        for j in range(2):
            r, s, t, slot = [row[2 * pair + j : 2 * pair + j + 1, :] for row in rows]
            weights.append((lagrange(r, nodes_ref), lagrange(s, nodes_ref)))
            weight_t = lagrange(t, nodes_ref)
            spread_t = [spread(weight_t[c : c + 1, :], 16) for c in range(8)]
            hots = [
                jnp.where(ids == spread(slot - float(16 * k), 16), jnp.ones((), BF16), zero)
                for k in range(elements // 16)
            ]
            columns_of.append(jnp.concatenate([hot * weight for weight in spread_t for hot in hots], axis=0))
        picker = jnp.concatenate(columns_of, axis=1)
        along = jnp.dot(fields_ref[...], picker, preferred_element_type=F32)
        for j in range(2):
            weight_r, weight_s = weights[j]
            columns = slice(j * LANES, (j + 1) * LANES)
            factors = [jnp.broadcast_to(weight_r[a : a + 1, :], (8, LANES)) for a in range(8)]
            for f in range(4):
                total = along[f * 64 : f * 64 + 8, columns] * factors[0]
                for a in range(1, 8):
                    total += along[f * 64 + a * 8 : f * 64 + a * 8 + 8, columns] * factors[a]
                pieces[f].append(jnp.sum(total * weight_s, axis=0, keepdims=True))
    return [jnp.concatenate(piece, axis=0) for piece in pieces]


def sample_kernel(
    sizes,
    rank_hbm,
    coords_hbm,
    slot_hbm,
    fields_hbm,
    part_ref,
    late_ref,
    block_ref,
    lane_ref,
    ids_ref,
    acc_ref,
    spaced_ref,
    turned_ref,
    table_ref,
    nodes_ref,
    rank_ref,
    coords_ref,
    slot_ref,
    fields_ref,
    back_ref,
    send_ref,
    recv_ref,
    values_ref,
    load_sem,
    out_sem,
    in_sem,
    back_out_sem,
    back_in_sem,
):
    count = sizes[0] * sizes[1] * sizes[2]
    quads, half = count // QUAD, count // 2
    me = (lax.axis_index("gx") * sizes[1] + lax.axis_index("gy")) * sizes[2] + lax.axis_index("gz")
    order = served(sizes)
    own = jnp.int32(0)
    for i in range(1, count):
        own = jnp.where(me == order[i], i, own)
    mesh_ids = pl.DeviceIdType.MESH

    def peer(i):
        rank = order[i]
        return (rank // (sizes[1] * sizes[2]), (rank // sizes[2]) % sizes[1], rank % sizes[2])

    def to_others(first, last, act):
        for i in range(first, last):
            pl.when(own != i)(functools.partial(act, i))

    def send(source, target, sent, arrived, i):
        pltpu.make_async_remote_copy(
            src_ref=source.at[:, i],
            dst_ref=target.at[:, own],
            send_sem=sent.at[0],
            recv_sem=arrived.at[own // QUAD],
            device_id=peer(i),
            device_id_type=mesh_ids,
        ).start()

    def keep(source, target, arrived):
        pltpu.make_async_copy(source.at[:, own], target.at[:, own], arrived.at[own // QUAD]).start()

    def wait_for(many, buffer, sem):
        pltpu.make_async_copy(buffer.at[:, :many], buffer.at[:, :many], sem).wait()

    loads = [
        pltpu.make_async_copy(source, target, load_sem.at[k])
        for k, (source, target) in enumerate(
            [(rank_hbm, rank_ref), (coords_hbm, coords_ref), (slot_hbm, slot_ref), (fields_hbm, fields_ref)]
        )
    ]
    for load in loads:
        load.start()
    barrier = pltpu.get_barrier_semaphore()
    to_others(
        0,
        count,
        lambda i: pl.semaphore_signal(barrier, inc=1, device_id=peer(i), device_id_type=mesh_ids),
    )
    for i in range(count):
        spaced_ref[i : i + 1, :] = jnp.full((1, LANES), float(order[i]), F32)
    ids_ref[...] = spaced_ref[:count, :].astype(BF16)
    write_nodes(nodes_ref)
    loads[0].wait()
    place(count, rank_ref, ids_ref, block_ref, lane_ref)
    loads[1].wait()
    loads[2].wait()
    for part in (0, 1):
        scatter(
            part * half, half, rank_ref, coords_ref, slot_ref, block_ref, lane_ref, ids_ref, send_ref, acc_ref
        )
        if part == 0:
            pl.semaphore_wait(barrier, count - 1)
        to_others(part * half, (part + 1) * half, functools.partial(send, send_ref, recv_ref, out_sem, in_sem))
    keep(send_ref, recv_ref, in_sem)
    loads[3].wait()
    turn_fields(fields_ref, spaced_ref, turned_ref)

    def body(quad, _):
        wait_for(QUAD, recv_ref, in_sem.at[quad])
        for turn in range(5):
            spots = []
            for m in range(4):
                row = pl.multiple_of(quad * QUAD + 8 * (turn if turn < 4 else m), 8)
                spots.append((m if turn < 4 else 4, pl.ds(row, 8)))
            rows = swap_groups([recv_ref[b, at, :] for b, at in spots])
            values = swap_groups(interpolate(rows, turned_ref, nodes_ref))
            for (b, at), value in zip(spots, values):
                values_ref[b, at, :] = value

        for g in range(quads):

            @pl.when(quad == g)
            def _():
                to_others(
                    QUAD * g,
                    QUAD * g + QUAD,
                    functools.partial(send, values_ref, back_ref, back_out_sem, back_in_sem),
                )

        return 0

    lax.fori_loop(0, quads, body, 0)
    keep(values_ref, back_ref, back_in_sem)
    early = count - QUAD
    for quad in range(quads - 1):
        wait_for(QUAD, back_ref, back_in_sem.at[quad])
    rows = [back_ref[b, :early, :] for b in range(BLOCKS)]
    rows.append(jnp.zeros((-BLOCKS * early % LANES, LANES), F32))
    table_ref[...] = jnp.concatenate(rows, axis=0).T.astype(BF16)
    pick(table_ref, ids_ref[:early, :], rank_ref, block_ref, lane_ref, None, part_ref)
    wait_for(QUAD, back_ref, back_in_sem.at[quads - 1])
    for b in range(BLOCKS):
        late_ref[b * QUAD : (b + 1) * QUAD, :] = back_ref[b, early:, :]
    wait_for(count - 1, send_ref, out_sem.at[0])
    wait_for(count - 1, values_ref, back_out_sem.at[0])


def pick(table_ref, ids, rank_ref, block_ref, lane_ref, part_ref, out_ref):
    probes = rank_ref.shape[1]
    ids = twice(ids)
    lane_ids = lax.broadcasted_iota(jnp.int32, (PIECE, CHUNK), 0).astype(F32)

    def body(step, _):
        for g in range(RETURNED):
            at = chunk_at(step, g, RETURNED)
            rank, block = rank_ref[:, at].astype(F32), block_ref[:, at]
            hots = [one_hot(ids, jnp.where(block == float(b), rank, -1.0)) for b in range(BLOCKS)]
            spare = table_ref.shape[1] - BLOCKS * ids.shape[0]
            if spare:
                hots.append(jnp.zeros((spare, CHUNK), BF16))
            picked = jnp.dot(table_ref[...], jnp.concatenate(hots, axis=0), preferred_element_type=F32)
            here = lane_ids == jnp.broadcast_to(lane_ref[:, at], (PIECE, CHUNK))
            for f in range(4):
                value = jnp.sum(
                    jnp.where(here, picked[f * PIECE : (f + 1) * PIECE], 0.0), axis=0, keepdims=True
                )
                out_ref[f : f + 1, at] = value if part_ref is None else value + part_ref[f : f + 1, at]
        return 0

    lax.fori_loop(0, probes // (RETURNED * CHUNK), body, 0)


def return_kernel(late_ref, part_ref, rank_ref, block_ref, lane_ref, ids_ref, out_ref, table_ref):
    late = late_ref.shape[0]
    rows = jnp.concatenate([late_ref[...], jnp.zeros((-late % LANES, LANES), F32)], axis=0)
    table_ref[...] = rows.T.astype(BF16)
    pick(table_ref, ids_ref[-(late // BLOCKS) :, :], rank_ref, block_ref, lane_ref, part_ref, out_ref)


VMEM = pl.BlockSpec(memory_space=pltpu.VMEM)
HBM = pl.BlockSpec(memory_space=pltpu.HBM)


def call(kernel, inputs, outputs, scratch, **options):
    return pl.pallas_call(
        kernel,
        out_shape=outputs,
        in_specs=inputs,
        out_specs=jax.tree.map(lambda _: VMEM, outputs),
        scratch_shapes=scratch,
        compiler_params=pltpu.CompilerParams(vmem_limit_bytes=48 << 20, **options),
    )


def local(sizes, fields, coordinates, element_rank, element_slot):
    count = sizes[0] * sizes[1] * sizes[2]
    probes = element_slot.shape[0]
    elements = fields.shape[0]
    line = jax.ShapeDtypeStruct((1, probes), F32)

    buffer = pltpu.VMEM((BLOCKS, count, LANES), F32)
    rank = element_rank.reshape(1, probes)
    late = BLOCKS * QUAD
    whole = jax.ShapeDtypeStruct((4, probes), F32)
    part, returned, block, lane, ids = call(
        functools.partial(sample_kernel, sizes),
        [HBM] * 4,
        (
            whole,
            jax.ShapeDtypeStruct((late, LANES), F32),
            line,
            line,
            jax.ShapeDtypeStruct((count, LANES), BF16),
        ),
        [
            pltpu.VMEM((BLOCKS * count // 2, 2 * LANES), F32),
            pltpu.VMEM((256 * 8, elements), F32),
            pltpu.VMEM((256, 8 * elements), BF16),
            pltpu.VMEM((LANES, -(-BLOCKS * (count - QUAD) // LANES) * LANES), BF16),
        ]
        + [
            pltpu.VMEM((64, LANES), F32),
            pltpu.VMEM(rank.shape, jnp.int32),
            pltpu.VMEM(coordinates.shape, F32),
            pltpu.VMEM(rank.shape, jnp.int32),
            pltpu.VMEM(fields.shape, BF16),
        ]
        + [buffer] * 4
        + [pltpu.SemaphoreType.DMA((n,)) for n in (4, 1, count // QUAD, 1, count // QUAD)],
        collective_id=0,
        has_side_effects=True,
    )(
        *[
            pltpu.with_memory_space_constraint(array, pltpu.HBM)
            for array in (rank, coordinates, element_slot.reshape(1, probes), fields)
        ]
    )
    return call(
        return_kernel,
        [VMEM] * 6,
        whole,
        [pltpu.VMEM((LANES, -(-late // LANES) * LANES), BF16)],
    )(returned, part, rank, block, lane, ids)


def solution(mesh):
    sizes = tuple(mesh.shape[axis] for axis in AXES)
    placed = (P(AXES, None), P(None, AXES), P(AXES, None), P(AXES))
    return jax.shard_map(
        functools.partial(local, sizes),
        mesh=mesh,
        in_specs=placed,
        out_specs=P(None, AXES),
        check_vma=False,
    )
```

```python
import functools

import jax
import jax.numpy as jnp
import numpy as np
from jax import lax
from jax.experimental import pallas as pl
from jax.experimental.pallas import tpu as pltpu
from jax.sharding import PartitionSpec as P

AXES = ("gx", "gy", "gz")
F32, BF16 = jnp.float32, jnp.bfloat16
LANES = 128
CHUNK = 256
PIECE = 32
BLOCKS = 5
QUAD = 32
PLACED = 32
GATHERED = 32
RETURNED = 32

gll_points = np.array(
    [
        -1.0,
        -0.8717401485096066,
        -0.5917001814331423,
        -0.2092992179024789,
        0.2092992179024789,
        0.5917001814331423,
        0.8717401485096066,
        1.0,
    ]
)
gll_scale = np.array(
    [1.0 / np.prod([gll_points[a] - gll_points[b] for b in range(8) if b != a]) for a in range(8)]
)
node_table = np.stack([gll_scale] + [np.roll(gll_points, -k) for k in range(1, 8)], axis=0)

REACHED = ((0.0, 1.1, 1.2, 1.6), (0.0, 1.3, 1.5, 1.8), (0.0, 1.5, 2.3, 2.8))


def served(sizes):
    def reached(rank):
        x, y, z = rank // (sizes[1] * sizes[2]), (rank // sizes[2]) % sizes[1], rank % sizes[2] // 2
        return REACHED[0][x] + REACHED[1][y] + REACHED[2][z]

    return sorted(range(sizes[0] * sizes[1] * sizes[2]), key=lambda rank: (reached(rank), rank))


def iota_bf16(shape):
    return lax.broadcasted_iota(jnp.int32, shape, 0).astype(F32).astype(BF16)


def spread(row, count):
    return jnp.broadcast_to(row, (count, row.shape[1])).astype(BF16)


def one_hot(ids, row):
    return jnp.where(ids == spread(row, ids.shape[0]), jnp.ones((), BF16), jnp.zeros((), BF16))


def twice(ids):
    return jnp.concatenate([ids, ids], axis=1)


def chunk_at(step, g, group):
    return pl.ds(pl.multiple_of((step * group + g) * CHUNK, CHUNK), CHUNK)


def place(count, rank_ref, ids_ref, block_ref, lane_ref):
    probes = rank_ref.shape[1]
    ids = twice(ids_ref[...])
    before = lax.broadcasted_iota(jnp.int32, (CHUNK, CHUNK), 0) <= lax.broadcasted_iota(jnp.int32, (CHUNK, CHUNK), 1)
    prefix = jnp.where(before, 1.0, 0.0).astype(BF16)

    def body(step, carry):
        hots = [one_hot(ids, rank_ref[:, chunk_at(step, g, PLACED)].astype(F32)) for g in range(PLACED)]
        counted = jnp.dot(jnp.concatenate(hots, axis=0), prefix, preferred_element_type=F32)
        for g in range(PLACED):
            at = chunk_at(step, g, PLACED)
            piece = counted[g * count : (g + 1) * count].astype(BF16)
            inside = (piece + twice(carry)) * hots[g]
            total = inside[:16]
            for k in range(1, count // 16):
                total = total + inside[16 * k : 16 * k + 16]
            position = jnp.sum(total.astype(F32), axis=0, keepdims=True) - 1.0
            block = jnp.floor(position * (1.0 / PIECE))
            lane_ref[:, at] = position - block * PIECE
            block_ref[:, at] = block
            carry = carry + jnp.broadcast_to(piece[:, CHUNK - 1 :], carry.shape)
        return carry

    lax.fori_loop(0, probes // (CHUNK * PLACED), body, jnp.zeros((count, LANES), BF16))


def scatter(rank_ref, coords_ref, slot_ref, block_ref, lane_ref, ids_ref, send_ref, acc_ref):
    probes = rank_ref.shape[1]
    many = ids_ref.shape[0]
    ids = twice(ids_ref[...])
    lane_ids = iota_bf16((PIECE, CHUNK))
    zero = jnp.zeros((), BF16)
    acc_ref[...] = jnp.zeros_like(acc_ref)

    def body(step, _):
        row_hots, lane_parts = [], []
        for g in range(GATHERED):
            at = chunk_at(step, g, GATHERED)
            rank, block, lane = rank_ref[:, at].astype(F32), block_ref[:, at], lane_ref[:, at]
            row_hots.append(
                jnp.concatenate(
                    [one_hot(ids, jnp.where(block == float(b), rank, -1.0)) for b in range(BLOCKS)], axis=0
                )
            )
            here = lane_ids == spread(lane, PIECE)
            high, low = [], []
            for v in range(3):
                value = coords_ref[v : v + 1, at]
                top = value.astype(BF16).astype(F32)
                high.append(top)
                low.append(value - top)
            high.append(slot_ref[:, at].astype(F32))
            chosen = [jnp.where(here, spread(part, PIECE), zero) for part in high + low]
            chosen.append(jnp.zeros((PIECE, CHUNK), BF16))
            lane_parts.append(jnp.concatenate(chosen, axis=0))
        acc_ref[...] += lax.dot_general(
            jnp.concatenate(row_hots, axis=1),
            jnp.concatenate(lane_parts, axis=1),
            (((1,), (1,)), ((), ())),
            preferred_element_type=F32,
        )
        return 0

    lax.fori_loop(0, probes // (GATHERED * CHUNK), body, 0)
    for b in range(BLOCKS):
        rows = slice(b * many, (b + 1) * many)
        send_ref[b] = acc_ref[rows, :LANES] + acc_ref[rows, LANES:]


def swap_groups(rows):
    lane = lax.broadcasted_iota(jnp.int32, (8, LANES), 1)
    for width in (2, 1):
        shift = width * PIECE
        lower = (lane // shift) % 2 == 0
        swapped = list(rows)
        for k in range(4):
            if (k // width) % 2 == 0:
                a, b = rows[k], rows[k + width]
                swapped[k] = jnp.where(lower, a, pltpu.roll(b, shift, 1))
                swapped[k + width] = jnp.where(lower, pltpu.roll(a, LANES - shift, 1), b)
        rows = swapped
    return rows


def write_nodes(nodes_ref):
    row = lax.broadcasted_iota(jnp.int32, (8, LANES), 0)
    for k in range(8):
        value = jnp.full((8, LANES), float(node_table[k, 0]), F32)
        for a in range(1, 8):
            value = jnp.where(row == a, float(node_table[k, a]), value)
        nodes_ref[8 * k : 8 * k + 8, :] = value


def turn_fields(fields_ref, spaced_ref, turned_ref):
    elements = fields_ref.shape[0]
    for k in range(fields_ref.shape[1] // LANES):
        spaced_ref[k * LANES : (k + 1) * LANES, :] = fields_ref[:, k * LANES : (k + 1) * LANES].astype(F32).T
    for c in range(8):
        turned_ref[:, c * elements : (c + 1) * elements] = spaced_ref[pl.ds(c, 256, stride=8), :].astype(BF16)


def lagrange(coord, nodes_ref):
    weight = nodes_ref[0:8, :]
    spread_coord = jnp.broadcast_to(coord, (8, LANES))
    for k in range(1, 8):
        weight = weight * (spread_coord - nodes_ref[8 * k : 8 * k + 8, :])
    return weight


def interpolate(rows, fields_ref, nodes_ref):
    depth = fields_ref.shape[1]
    elements = depth // 8
    zero = jnp.zeros((), BF16)
    ids = iota_bf16((16, LANES))
    pieces = [[] for _ in range(4)]
    for pair in range(len(rows[0]) // 2):
        weights, columns_of = [], []
        for j in range(2):
            r, s, t, slot = [row[2 * pair + j : 2 * pair + j + 1, :] for row in rows]
            weights.append((lagrange(r, nodes_ref), lagrange(s, nodes_ref)))
            weight_t = lagrange(t, nodes_ref)
            spread_t = [spread(weight_t[c : c + 1, :], 16) for c in range(8)]
            hots = [
                jnp.where(ids == spread(slot - float(16 * k), 16), jnp.ones((), BF16), zero)
                for k in range(elements // 16)
            ]
            columns_of.append(jnp.concatenate([hot * weight for weight in spread_t for hot in hots], axis=0))
        picker = jnp.concatenate(columns_of, axis=1)
        along = jnp.dot(fields_ref[...], picker, preferred_element_type=F32)
        for j in range(2):
            weight_r, weight_s = weights[j]
            columns = slice(j * LANES, (j + 1) * LANES)
            factors = [jnp.broadcast_to(weight_r[a : a + 1, :], (8, LANES)) for a in range(8)]
            for f in range(4):
                total = along[f * 64 : f * 64 + 8, columns] * factors[0]
                for a in range(1, 8):
                    total += along[f * 64 + a * 8 : f * 64 + a * 8 + 8, columns] * factors[a]
                pieces[f].append(jnp.sum(total * weight_s, axis=0, keepdims=True))
    return [jnp.concatenate(piece, axis=0) for piece in pieces]


def sample_kernel(
    sizes,
    rank_hbm,
    coords_hbm,
    slot_hbm,
    fields_hbm,
    part_ref,
    late_ref,
    block_ref,
    lane_ref,
    late_ids_ref,
    ids_ref,
    acc_ref,
    spaced_ref,
    turned_ref,
    table_ref,
    nodes_ref,
    rank_ref,
    coords_ref,
    slot_ref,
    fields_ref,
    back_ref,
    send_ref,
    recv_ref,
    values_ref,
    load_sem,
    out_sem,
    in_sem,
    back_out_sem,
    back_in_sem,
):
    count = sizes[0] * sizes[1] * sizes[2]
    quads, half = count // QUAD, count // 2
    me = (lax.axis_index("gx") * sizes[1] + lax.axis_index("gy")) * sizes[2] + lax.axis_index("gz")
    order = served(sizes)
    own = jnp.int32(0)
    for i in range(1, count):
        own = jnp.where(me == order[i], i, own)
    mesh_ids = pl.DeviceIdType.MESH

    def peer(i):
        rank = order[i]
        return (rank // (sizes[1] * sizes[2]), (rank // sizes[2]) % sizes[1], rank % sizes[2])

    def to_others(first, last, act):
        for i in range(first, last):
            pl.when(own != i)(functools.partial(act, i))

    def send(source, target, sent, arrived, i):
        pltpu.make_async_remote_copy(
            src_ref=source.at[:, i],
            dst_ref=target.at[:, own],
            send_sem=sent.at[0],
            recv_sem=arrived.at[own // QUAD],
            device_id=peer(i),
            device_id_type=mesh_ids,
        ).start()

    def keep(source, target, arrived):
        pltpu.make_async_copy(source.at[:, own], target.at[:, own], arrived.at[own // QUAD]).start()

    def wait_for(many, buffer, sem):
        pltpu.make_async_copy(buffer.at[:, :many], buffer.at[:, :many], sem).wait()

    loads = [
        pltpu.make_async_copy(source, target, load_sem.at[k])
        for k, (source, target) in enumerate(
            [(rank_hbm, rank_ref), (coords_hbm, coords_ref), (slot_hbm, slot_ref), (fields_hbm, fields_ref)]
        )
    ]
    for load in loads:
        load.start()
    barrier = pltpu.get_barrier_semaphore()
    to_others(
        0,
        count,
        lambda i: pl.semaphore_signal(barrier, inc=1, device_id=peer(i), device_id_type=mesh_ids),
    )
    for i in range(count):
        spaced_ref[i : i + 1, :] = jnp.full((1, LANES), float(order[i]), F32)
    ids_ref[...] = spaced_ref[:count, :].astype(BF16)
    write_nodes(nodes_ref)
    loads[0].wait()
    place(count, rank_ref, ids_ref, block_ref, lane_ref)
    loads[1].wait()
    loads[2].wait()
    scatter(rank_ref, coords_ref, slot_ref, block_ref, lane_ref, ids_ref, send_ref, acc_ref)
    pl.semaphore_wait(barrier, count - 1)

    def ask(phase, _):
        for h in range(2):

            @pl.when((phase + own // QUAD) % 2 == h)
            def _():
                to_others(h * half, (h + 1) * half, functools.partial(send, send_ref, recv_ref, out_sem, in_sem))

        return 0

    lax.fori_loop(0, 2, ask, 0)
    keep(send_ref, recv_ref, in_sem)
    loads[3].wait()
    turn_fields(fields_ref, spaced_ref, turned_ref)

    side = own // half

    def body(step, _):
        quad = step + side * (1 - 2 * (step % 2))
        wait_for(QUAD, recv_ref, in_sem.at[quad])
        for turn in range(5):
            spots = []
            for m in range(4):
                row = pl.multiple_of(quad * QUAD + 8 * (turn if turn < 4 else m), 8)
                spots.append((m if turn < 4 else 4, pl.ds(row, 8)))
            rows = swap_groups([recv_ref[b, at, :] for b, at in spots])
            values = swap_groups(interpolate(rows, turned_ref, nodes_ref))
            for (b, at), value in zip(spots, values):
                values_ref[b, at, :] = value

        for g in range(quads):

            @pl.when(quad == g)
            def _():
                to_others(
                    QUAD * g,
                    QUAD * g + QUAD,
                    functools.partial(send, values_ref, back_ref, back_out_sem, back_in_sem),
                )

        return 0

    lax.fori_loop(0, quads, body, 0)
    keep(values_ref, back_ref, back_in_sem)
    first = own // QUAD % 2
    table_ref[...] = answers(first, half, back_ref, functools.partial(wait_for, QUAD), back_in_sem).T.astype(BF16)
    pick(table_ref, ids_ref[halves(first, half), :], rank_ref, block_ref, lane_ref, None, part_ref)
    late_ref[...] = answers(1 - first, half, back_ref, functools.partial(wait_for, QUAD), back_in_sem)
    late_ids_ref[...] = ids_ref[halves(1 - first, half), :]
    wait_for(count - 1, send_ref, out_sem.at[0])
    wait_for(count - 1, values_ref, back_out_sem.at[0])


def halves(which, half):
    return pl.ds(pl.multiple_of(which * half, half), half)


def answers(which, half, back_ref, wait, back_in_sem):
    for k in range(half // QUAD):
        wait(back_ref, back_in_sem.at[which * (half // QUAD) + k])
    rows = [back_ref[b, halves(which, half), :] for b in range(BLOCKS)]
    rows.append(jnp.zeros((-BLOCKS * half % LANES, LANES), F32))
    return jnp.concatenate(rows, axis=0)


def pick(table_ref, ids, rank_ref, block_ref, lane_ref, part_ref, out_ref):
    probes = rank_ref.shape[1]
    ids = twice(ids)
    lane_ids = lax.broadcasted_iota(jnp.int32, (PIECE, CHUNK), 0).astype(F32)

    def body(step, _):
        for g in range(RETURNED):
            at = chunk_at(step, g, RETURNED)
            rank, block = rank_ref[:, at].astype(F32), block_ref[:, at]
            hots = [one_hot(ids, jnp.where(block == float(b), rank, -1.0)) for b in range(BLOCKS)]
            spare = table_ref.shape[1] - BLOCKS * ids.shape[0]
            if spare:
                hots.append(jnp.zeros((spare, CHUNK), BF16))
            picked = jnp.dot(table_ref[...], jnp.concatenate(hots, axis=0), preferred_element_type=F32)
            here = lane_ids == jnp.broadcast_to(lane_ref[:, at], (PIECE, CHUNK))
            for f in range(4):
                value = jnp.sum(
                    jnp.where(here, picked[f * PIECE : (f + 1) * PIECE], 0.0), axis=0, keepdims=True
                )
                out_ref[f : f + 1, at] = value if part_ref is None else value + part_ref[f : f + 1, at]
        return 0

    lax.fori_loop(0, probes // (RETURNED * CHUNK), body, 0)


def return_kernel(late_ref, part_ref, rank_ref, block_ref, lane_ref, ids_ref, out_ref, table_ref):
    table_ref[...] = late_ref[...].T.astype(BF16)
    pick(table_ref, ids_ref[...], rank_ref, block_ref, lane_ref, part_ref, out_ref)


VMEM = pl.BlockSpec(memory_space=pltpu.VMEM)
HBM = pl.BlockSpec(memory_space=pltpu.HBM)


def call(kernel, inputs, outputs, scratch, **options):
    return pl.pallas_call(
        kernel,
        out_shape=outputs,
        in_specs=inputs,
        out_specs=jax.tree.map(lambda _: VMEM, outputs),
        scratch_shapes=scratch,
        compiler_params=pltpu.CompilerParams(vmem_limit_bytes=48 << 20, **options),
    )


def local(sizes, fields, coordinates, element_rank, element_slot):
    count = sizes[0] * sizes[1] * sizes[2]
    probes = element_slot.shape[0]
    elements = fields.shape[0]
    line = jax.ShapeDtypeStruct((1, probes), F32)

    buffer = pltpu.VMEM((BLOCKS, count, LANES), F32)
    rank = element_rank.reshape(1, probes)
    late = -(-BLOCKS * (count // 2) // LANES) * LANES
    whole = jax.ShapeDtypeStruct((4, probes), F32)
    part, returned, block, lane, ids = call(
        functools.partial(sample_kernel, sizes),
        [HBM] * 4,
        (
            whole,
            jax.ShapeDtypeStruct((late, LANES), F32),
            line,
            line,
            jax.ShapeDtypeStruct((count // 2, LANES), BF16),
        ),
        [
            pltpu.VMEM((count, LANES), BF16),
            pltpu.VMEM((BLOCKS * count, 2 * LANES), F32),
            pltpu.VMEM((256 * 8, elements), F32),
            pltpu.VMEM((256, 8 * elements), BF16),
            pltpu.VMEM((LANES, late), BF16),
        ]
        + [
            pltpu.VMEM((64, LANES), F32),
            pltpu.VMEM(rank.shape, jnp.int32),
            pltpu.VMEM(coordinates.shape, F32),
            pltpu.VMEM(rank.shape, jnp.int32),
            pltpu.VMEM(fields.shape, BF16),
        ]
        + [buffer] * 4
        + [pltpu.SemaphoreType.DMA((n,)) for n in (4, 1, count // QUAD, 1, count // QUAD)],
        collective_id=0,
        has_side_effects=True,
    )(
        *[
            pltpu.with_memory_space_constraint(array, pltpu.HBM)
            for array in (rank, coordinates, element_slot.reshape(1, probes), fields)
        ]
    )
    return call(
        return_kernel,
        [VMEM] * 6,
        whole,
        [pltpu.VMEM((LANES, late), BF16)],
    )(returned, part, rank, block, lane, ids)


def solution(mesh):
    sizes = tuple(mesh.shape[axis] for axis in AXES)
    placed = (P(AXES, None), P(None, AXES), P(AXES, None), P(AXES))
    return jax.shard_map(
        functools.partial(local, sizes),
        mesh=mesh,
        in_specs=placed,
        out_specs=P(None, AXES),
        check_vma=False,
    )
```

```python
import functools

import jax
import jax.numpy as jnp
import numpy as np
from jax import lax
from jax.experimental import pallas as pl
from jax.experimental.pallas import tpu as pltpu
from jax.sharding import PartitionSpec as P

AXES = ("gx", "gy", "gz")
F32, BF16 = jnp.float32, jnp.bfloat16
LANES = 128
CHUNK = 256
PIECE = 32
BLOCKS = 5
QUAD = 32
PLACED = 32
GATHERED = 32
RETURNED = 32

gll_points = np.array(
    [
        -1.0,
        -0.8717401485096066,
        -0.5917001814331423,
        -0.2092992179024789,
        0.2092992179024789,
        0.5917001814331423,
        0.8717401485096066,
        1.0,
    ]
)
gll_scale = np.array(
    [1.0 / np.prod([gll_points[a] - gll_points[b] for b in range(8) if b != a]) for a in range(8)]
)
node_table = np.stack([gll_scale] + [np.roll(gll_points, -k) for k in range(1, 8)], axis=0)

REACHED = ((0.0, 1.1, 1.2, 1.6), (0.0, 1.3, 1.5, 1.8), (0.0, 1.5, 2.3, 2.8))


def served(sizes):
    def reached(rank):
        x, y, z = rank // (sizes[1] * sizes[2]), (rank // sizes[2]) % sizes[1], rank % sizes[2] // 2
        return REACHED[0][x] + REACHED[1][y] + REACHED[2][z]

    return sorted(range(sizes[0] * sizes[1] * sizes[2]), key=lambda rank: (reached(rank), rank))


def iota_bf16(shape):
    return lax.broadcasted_iota(jnp.int32, shape, 0).astype(F32).astype(BF16)


def spread(row, count):
    return jnp.broadcast_to(row, (count, row.shape[1])).astype(BF16)


def one_hot(ids, row):
    return jnp.where(ids == spread(row, ids.shape[0]), jnp.ones((), BF16), jnp.zeros((), BF16))


def twice(ids):
    return jnp.concatenate([ids, ids], axis=1)


def chunk_at(step, g, group):
    return pl.ds(pl.multiple_of((step * group + g) * CHUNK, CHUNK), CHUNK)


def place(count, rank_ref, ids_ref, block_ref, lane_ref):
    probes = rank_ref.shape[1]
    ids = twice(ids_ref[...])
    before = lax.broadcasted_iota(jnp.int32, (CHUNK, CHUNK), 0) <= lax.broadcasted_iota(jnp.int32, (CHUNK, CHUNK), 1)
    prefix = jnp.where(before, 1.0, 0.0).astype(BF16)

    def body(step, carry):
        hots = [one_hot(ids, rank_ref[:, chunk_at(step, g, PLACED)].astype(F32)) for g in range(PLACED)]
        counted = jnp.dot(jnp.concatenate(hots, axis=0), prefix, preferred_element_type=F32)
        for g in range(PLACED):
            at = chunk_at(step, g, PLACED)
            piece = counted[g * count : (g + 1) * count].astype(BF16)
            inside = (piece + twice(carry)) * hots[g]
            total = inside[:16]
            for k in range(1, count // 16):
                total = total + inside[16 * k : 16 * k + 16]
            position = jnp.sum(total.astype(F32), axis=0, keepdims=True) - 1.0
            block = jnp.floor(position * (1.0 / PIECE))
            lane_ref[:, at] = position - block * PIECE
            block_ref[:, at] = block
            carry = carry + jnp.broadcast_to(piece[:, CHUNK - 1 :], carry.shape)
        return carry

    lax.fori_loop(0, probes // (CHUNK * PLACED), body, jnp.zeros((count, LANES), BF16))


def scatter(rank_ref, coords_ref, slot_ref, block_ref, lane_ref, ids_ref, send_ref, acc_ref):
    probes = rank_ref.shape[1]
    many = ids_ref.shape[0]
    ids = twice(ids_ref[...])
    lane_ids = iota_bf16((PIECE, CHUNK))
    zero = jnp.zeros((), BF16)
    acc_ref[...] = jnp.zeros_like(acc_ref)

    def body(step, _):
        row_hots, lane_parts = [], []
        for g in range(GATHERED):
            at = chunk_at(step, g, GATHERED)
            rank, block, lane = rank_ref[:, at].astype(F32), block_ref[:, at], lane_ref[:, at]
            row_hots.append(
                jnp.concatenate(
                    [one_hot(ids, jnp.where(block == float(b), rank, -1.0)) for b in range(BLOCKS)], axis=0
                )
            )
            here = lane_ids == spread(lane, PIECE)
            high, low = [], []
            for v in range(3):
                value = coords_ref[v : v + 1, at]
                top = value.astype(BF16).astype(F32)
                high.append(top)
                low.append(value - top)
            high.append(slot_ref[:, at].astype(F32))
            chosen = [jnp.where(here, spread(part, PIECE), zero) for part in high + low]
            chosen.append(jnp.zeros((PIECE, CHUNK), BF16))
            lane_parts.append(jnp.concatenate(chosen, axis=0))
        acc_ref[...] += lax.dot_general(
            jnp.concatenate(row_hots, axis=1),
            jnp.concatenate(lane_parts, axis=1),
            (((1,), (1,)), ((), ())),
            preferred_element_type=F32,
        )
        return 0

    lax.fori_loop(0, probes // (GATHERED * CHUNK), body, 0)
    for b in range(BLOCKS):
        rows = slice(b * many, (b + 1) * many)
        send_ref[b] = acc_ref[rows, :LANES] + acc_ref[rows, LANES:]


def swap_groups(rows):
    lane = lax.broadcasted_iota(jnp.int32, (8, LANES), 1)
    for width in (2, 1):
        shift = width * PIECE
        lower = (lane // shift) % 2 == 0
        swapped = list(rows)
        for k in range(4):
            if (k // width) % 2 == 0:
                a, b = rows[k], rows[k + width]
                swapped[k] = jnp.where(lower, a, pltpu.roll(b, shift, 1))
                swapped[k + width] = jnp.where(lower, pltpu.roll(a, LANES - shift, 1), b)
        rows = swapped
    return rows


def write_nodes(nodes_ref):
    row = lax.broadcasted_iota(jnp.int32, (8, LANES), 0)
    for k in range(8):
        value = jnp.full((8, LANES), float(node_table[k, 0]), F32)
        for a in range(1, 8):
            value = jnp.where(row == a, float(node_table[k, a]), value)
        nodes_ref[8 * k : 8 * k + 8, :] = value


def turn_fields(fields_ref, spaced_ref, turned_ref):
    elements = fields_ref.shape[0]
    for k in range(fields_ref.shape[1] // LANES):
        spaced_ref[k * LANES : (k + 1) * LANES, :] = fields_ref[:, k * LANES : (k + 1) * LANES].astype(F32).T
    for c in range(8):
        turned_ref[:, c * elements : (c + 1) * elements] = spaced_ref[pl.ds(c, 256, stride=8), :].astype(BF16)


def lagrange(coord, nodes_ref):
    weight = nodes_ref[0:8, :]
    spread_coord = jnp.broadcast_to(coord, (8, LANES))
    for k in range(1, 8):
        weight = weight * (spread_coord - nodes_ref[8 * k : 8 * k + 8, :])
    return weight


def interpolate(rows, fields_ref, nodes_ref):
    depth = fields_ref.shape[1]
    elements = depth // 8
    zero = jnp.zeros((), BF16)
    ids = iota_bf16((16, LANES))
    pieces = [[] for _ in range(4)]
    for pair in range(len(rows[0]) // 2):
        weights, columns_of = [], []
        for j in range(2):
            r, s, t, slot = [row[2 * pair + j : 2 * pair + j + 1, :] for row in rows]
            weights.append((lagrange(r, nodes_ref), lagrange(s, nodes_ref)))
            weight_t = lagrange(t, nodes_ref)
            spread_t = [spread(weight_t[c : c + 1, :], 16) for c in range(8)]
            hots = [
                jnp.where(ids == spread(slot - float(16 * k), 16), jnp.ones((), BF16), zero)
                for k in range(elements // 16)
            ]
            columns_of.append(jnp.concatenate([hot * weight for weight in spread_t for hot in hots], axis=0))
        picker = jnp.concatenate(columns_of, axis=1)
        along = jnp.dot(fields_ref[...], picker, preferred_element_type=F32)
        for j in range(2):
            weight_r, weight_s = weights[j]
            columns = slice(j * LANES, (j + 1) * LANES)
            factors = [jnp.broadcast_to(weight_r[a : a + 1, :], (8, LANES)) for a in range(8)]
            for f in range(4):
                total = along[f * 64 : f * 64 + 8, columns] * factors[0]
                for a in range(1, 8):
                    total += along[f * 64 + a * 8 : f * 64 + a * 8 + 8, columns] * factors[a]
                pieces[f].append(jnp.sum(total * weight_s, axis=0, keepdims=True))
    return [jnp.concatenate(piece, axis=0) for piece in pieces]


def sample_kernel(
    sizes,
    rank_hbm,
    coords_hbm,
    slot_hbm,
    fields_hbm,
    part_ref,
    late_ref,
    block_ref,
    lane_ref,
    ids_ref,
    acc_ref,
    spaced_ref,
    turned_ref,
    table_ref,
    nodes_ref,
    rank_ref,
    coords_ref,
    slot_ref,
    fields_ref,
    back_ref,
    send_ref,
    recv_ref,
    values_ref,
    load_sem,
    out_sem,
    in_sem,
    back_out_sem,
    back_in_sem,
):
    count = sizes[0] * sizes[1] * sizes[2]
    quads, half = count // QUAD, count // 2
    me = (lax.axis_index("gx") * sizes[1] + lax.axis_index("gy")) * sizes[2] + lax.axis_index("gz")
    order = served(sizes)
    own = jnp.int32(0)
    for i in range(1, count):
        own = jnp.where(me == order[i], i, own)
    mesh_ids = pl.DeviceIdType.MESH

    def peer(i):
        rank = order[i]
        return (rank // (sizes[1] * sizes[2]), (rank // sizes[2]) % sizes[1], rank % sizes[2])

    def to_others(first, last, act):
        for i in range(first, last):
            pl.when(own != i)(functools.partial(act, i))

    def send(source, target, sent, arrived, i):
        pltpu.make_async_remote_copy(
            src_ref=source.at[:, i],
            dst_ref=target.at[:, own],
            send_sem=sent.at[0],
            recv_sem=arrived.at[own // QUAD],
            device_id=peer(i),
            device_id_type=mesh_ids,
        ).start()

    def keep(source, target, arrived):
        pltpu.make_async_copy(source.at[:, own], target.at[:, own], arrived.at[own // QUAD]).start()

    def wait_for(many, buffer, sem):
        pltpu.make_async_copy(buffer.at[:, :many], buffer.at[:, :many], sem).wait()

    loads = [
        pltpu.make_async_copy(source, target, load_sem.at[k])
        for k, (source, target) in enumerate(
            [(rank_hbm, rank_ref), (coords_hbm, coords_ref), (slot_hbm, slot_ref), (fields_hbm, fields_ref)]
        )
    ]
    for load in loads:
        load.start()
    barrier = pltpu.get_barrier_semaphore()
    to_others(
        0,
        count,
        lambda i: pl.semaphore_signal(barrier, inc=1, device_id=peer(i), device_id_type=mesh_ids),
    )
    for i in range(count):
        spaced_ref[i : i + 1, :] = jnp.full((1, LANES), float(order[i]), F32)
    ids_ref[...] = spaced_ref[:count, :].astype(BF16)
    write_nodes(nodes_ref)
    loads[0].wait()
    place(count, rank_ref, ids_ref, block_ref, lane_ref)
    loads[1].wait()
    loads[2].wait()
    scatter(rank_ref, coords_ref, slot_ref, block_ref, lane_ref, ids_ref, send_ref, acc_ref)
    pl.semaphore_wait(barrier, count - 1)

    def ask(phase, _):
        for h in range(2):

            @pl.when((phase + own // QUAD) % 2 == h)
            def _():
                to_others(h * half, (h + 1) * half, functools.partial(send, send_ref, recv_ref, out_sem, in_sem))

        return 0

    lax.fori_loop(0, 2, ask, 0)
    keep(send_ref, recv_ref, in_sem)
    loads[3].wait()
    turn_fields(fields_ref, spaced_ref, turned_ref)

    side = own // (count - QUAD)

    def body(step, _):
        quad = step + side * (1 - 2 * (step % 2))
        wait_for(QUAD, recv_ref, in_sem.at[quad])
        for turn in range(5):
            spots = []
            for m in range(4):
                row = pl.multiple_of(quad * QUAD + 8 * (turn if turn < 4 else m), 8)
                spots.append((m if turn < 4 else 4, pl.ds(row, 8)))
            rows = swap_groups([recv_ref[b, at, :] for b, at in spots])
            values = swap_groups(interpolate(rows, turned_ref, nodes_ref))
            for (b, at), value in zip(spots, values):
                values_ref[b, at, :] = value

        for g in range(quads):

            @pl.when(quad == g)
            def _():
                to_others(
                    QUAD * g,
                    QUAD * g + QUAD,
                    functools.partial(send, values_ref, back_ref, back_out_sem, back_in_sem),
                )

        return 0

    lax.fori_loop(0, quads, body, 0)
    keep(values_ref, back_ref, back_in_sem)
    odd = own // QUAD % 2
    split = count - QUAD
    for flag, early, late in ((0, (0, split), (split, count)), (1, (split, count), (0, split))):

        @pl.when(odd == flag)
        def _():
            table = answers(early, back_ref, functools.partial(wait_for, QUAD), back_in_sem)
            table_ref[:, : table.shape[0]] = table.T.astype(BF16)
            pick(
                table_ref.at[:, : table.shape[0]], ids_ref[slice(*early), :], rank_ref, block_ref, lane_ref, None, part_ref
            )
            table = answers(late, back_ref, functools.partial(wait_for, QUAD), back_in_sem)
            late_ref[: table.shape[0], :] = table

    wait_for(count - 1, send_ref, out_sem.at[0])
    wait_for(count - 1, values_ref, back_out_sem.at[0])


def padded(many):
    return -(-BLOCKS * many // LANES) * LANES


def answers(span, back_ref, wait, back_in_sem):
    first, last = span
    for k in range(first // QUAD, last // QUAD):
        wait(back_ref, back_in_sem.at[k])
    rows = [back_ref[b, first:last, :] for b in range(BLOCKS)]
    rows.append(jnp.zeros((padded(last - first) - BLOCKS * (last - first), LANES), F32))
    return jnp.concatenate(rows, axis=0)


def pick(table_ref, ids, rank_ref, block_ref, lane_ref, part_ref, out_ref):
    probes = rank_ref.shape[1]
    ids = twice(ids)
    raised = ids + float(LANES)
    lane_ids = lax.broadcasted_iota(jnp.int32, (PIECE, CHUNK), 0).astype(F32)
    row_ids = lax.broadcasted_iota(jnp.int32, (8, CHUNK), 0)

    def merge(a, b, shift):
        lower = (row_ids // shift) % 2 == 0
        return jnp.where(lower, a, b) + pltpu.roll(jnp.where(lower, b, a), shift, 0)

    def body(step, _):
        for g in range(RETURNED):
            at = chunk_at(step, g, RETURNED)
            rank, block = rank_ref[:, at].astype(F32), block_ref[:, at]
            code = rank + block * float(LANES)
            hots = []
            for b in range(0, BLOCKS, 2):
                inside = (block >= float(b)) & (block < float(b + 2))
                row = jnp.where(inside, code - float(b * LANES), -1.0)
                hots += [one_hot(known, row) for known in (ids, raised)[: BLOCKS - b]]
            spare = table_ref.shape[1] - BLOCKS * ids.shape[0]
            if spare:
                hots.append(jnp.zeros((spare, CHUNK), BF16))
            picked = jnp.dot(table_ref[...], jnp.concatenate(hots, axis=0), preferred_element_type=F32)
            here = lane_ids == jnp.broadcast_to(lane_ref[:, at], (PIECE, CHUNK))
            sums = []
            for f in range(4):
                chosen = jnp.where(here, picked[f * PIECE : (f + 1) * PIECE], 0.0)
                sums.append(sum(chosen[8 * k : 8 * k + 8] for k in range(PIECE // 8)))
            mixed = merge(merge(sums[0], sums[1], 1), merge(sums[2], sums[3], 1), 2)
            value = (mixed + pltpu.roll(mixed, 4, 0))[:4]
            out_ref[:, at] = value if part_ref is None else value + part_ref[:, at]
        return 0

    lax.fori_loop(0, probes // (RETURNED * CHUNK), body, 0)


def return_kernel(sizes, late_ref, part_ref, rank_ref, block_ref, lane_ref, ids_ref, out_ref, table_ref):
    count = ids_ref.shape[0]
    own = (lax.axis_index("gx") * sizes[1] + lax.axis_index("gy")) * sizes[2] + lax.axis_index("gz")
    odd = jnp.int32(0)
    for i, rank in enumerate(served(sizes)):
        odd = jnp.where(own == rank, i // QUAD % 2, odd)
    split = count - QUAD
    for flag, (first, last) in enumerate(((split, count), (0, split))):

        @pl.when(odd == flag)
        def _():
            rows = padded(last - first)
            table_ref[:, :rows] = late_ref[:rows, :].T.astype(BF16)
            pick(table_ref.at[:, :rows], ids_ref[first:last, :], rank_ref, block_ref, lane_ref, part_ref, out_ref)


VMEM = pl.BlockSpec(memory_space=pltpu.VMEM)
HBM = pl.BlockSpec(memory_space=pltpu.HBM)


def call(kernel, inputs, outputs, scratch, **options):
    return pl.pallas_call(
        kernel,
        out_shape=outputs,
        in_specs=inputs,
        out_specs=jax.tree.map(lambda _: VMEM, outputs),
        scratch_shapes=scratch,
        compiler_params=pltpu.CompilerParams(vmem_limit_bytes=48 << 20, **options),
    )


def local(sizes, fields, coordinates, element_rank, element_slot):
    count = sizes[0] * sizes[1] * sizes[2]
    probes = element_slot.shape[0]
    elements = fields.shape[0]
    line = jax.ShapeDtypeStruct((1, probes), F32)

    buffer = pltpu.VMEM((BLOCKS, count, LANES), F32)
    rank = element_rank.reshape(1, probes)
    late = padded(count - QUAD)
    whole = jax.ShapeDtypeStruct((4, probes), F32)
    part, returned, block, lane, ids = call(
        functools.partial(sample_kernel, sizes),
        [HBM] * 4,
        (
            whole,
            jax.ShapeDtypeStruct((late, LANES), F32),
            line,
            line,
            jax.ShapeDtypeStruct((count, LANES), BF16),
        ),
        [
            pltpu.VMEM((BLOCKS * count, 2 * LANES), F32),
            pltpu.VMEM((256 * 8, elements), F32),
            pltpu.VMEM((256, 8 * elements), BF16),
            pltpu.VMEM((LANES, late), BF16),
        ]
        + [
            pltpu.VMEM((64, LANES), F32),
            pltpu.VMEM(rank.shape, jnp.int32),
            pltpu.VMEM(coordinates.shape, F32),
            pltpu.VMEM(rank.shape, jnp.int32),
            pltpu.VMEM(fields.shape, BF16),
        ]
        + [buffer] * 4
        + [pltpu.SemaphoreType.DMA((n,)) for n in (4, 1, count // QUAD, 1, count // QUAD)],
        collective_id=0,
        has_side_effects=True,
    )(
        *[
            pltpu.with_memory_space_constraint(array, pltpu.HBM)
            for array in (rank, coordinates, element_slot.reshape(1, probes), fields)
        ]
    )
    return call(
        functools.partial(return_kernel, sizes),
        [VMEM] * 6,
        whole,
        [pltpu.VMEM((LANES, late), BF16)],
    )(returned, part, rank, block, lane, ids)


def solution(mesh):
    sizes = tuple(mesh.shape[axis] for axis in AXES)
    placed = (P(AXES, None), P(None, AXES), P(AXES, None), P(AXES))
    return jax.shard_map(
        functools.partial(local, sizes),
        mesh=mesh,
        in_specs=placed,
        out_specs=P(None, AXES),
        check_vma=False,
    )
```

```python
import functools

import jax
import jax.numpy as jnp
import numpy as np
from jax import lax
from jax.experimental import pallas as pl
from jax.experimental.pallas import tpu as pltpu
from jax.sharding import PartitionSpec as P

AXES = ("gx", "gy", "gz")
F32, BF16 = jnp.float32, jnp.bfloat16
LANES = 128
CHUNK = 256
PIECE = 32
BLOCKS = 5
QUAD = 32
PLACED = 32
GATHERED = 32
RETURNED = 32

gll_points = np.array(
    [
        -1.0,
        -0.8717401485096066,
        -0.5917001814331423,
        -0.2092992179024789,
        0.2092992179024789,
        0.5917001814331423,
        0.8717401485096066,
        1.0,
    ]
)
gll_scale = np.array(
    [1.0 / np.prod([gll_points[a] - gll_points[b] for b in range(8) if b != a]) for a in range(8)]
)
node_table = np.stack([gll_scale] + [np.roll(gll_points, -k) for k in range(1, 8)], axis=0)

REACHED = ((0.0, 1.1, 1.2, 1.6), (0.0, 1.3, 1.5, 1.8), (0.0, 1.5, 2.3, 2.8))


def served(sizes):
    def reached(rank):
        x, y, z = rank // (sizes[1] * sizes[2]), (rank // sizes[2]) % sizes[1], rank % sizes[2] // 2
        return REACHED[0][x] + REACHED[1][y] + REACHED[2][z]

    return sorted(range(sizes[0] * sizes[1] * sizes[2]), key=lambda rank: (reached(rank), rank))


def iota_bf16(shape):
    return lax.broadcasted_iota(jnp.int32, shape, 0).astype(F32).astype(BF16)


def spread(row, count):
    return jnp.broadcast_to(row, (count, row.shape[1])).astype(BF16)


def one_hot(ids, row):
    return jnp.where(ids == spread(row, ids.shape[0]), jnp.ones((), BF16), jnp.zeros((), BF16))


def twice(ids):
    return jnp.concatenate([ids, ids], axis=1)


def chunk_at(step, g, group):
    return pl.ds(pl.multiple_of((step * group + g) * CHUNK, CHUNK), CHUNK)


def place(count, rank_ref, ids_ref, block_ref, lane_ref):
    probes = rank_ref.shape[1]
    ids = twice(ids_ref[...])
    before = lax.broadcasted_iota(jnp.int32, (CHUNK, CHUNK), 0) <= lax.broadcasted_iota(jnp.int32, (CHUNK, CHUNK), 1)
    prefix = jnp.where(before, 1.0, 0.0).astype(BF16)

    def body(step, carry):
        hots = [one_hot(ids, rank_ref[:, chunk_at(step, g, PLACED)].astype(F32)) for g in range(PLACED)]
        counted = jnp.dot(jnp.concatenate(hots, axis=0), prefix, preferred_element_type=F32)
        for g in range(PLACED):
            at = chunk_at(step, g, PLACED)
            piece = counted[g * count : (g + 1) * count].astype(BF16)
            inside = (piece + twice(carry)) * hots[g]
            total = inside[:16]
            for k in range(1, count // 16):
                total = total + inside[16 * k : 16 * k + 16]
            position = jnp.sum(total.astype(F32), axis=0, keepdims=True) - 1.0
            block = jnp.floor(position * (1.0 / PIECE))
            lane_ref[:, at] = position - block * PIECE
            block_ref[:, at] = block
            carry = carry + jnp.broadcast_to(piece[:, CHUNK - 1 :], carry.shape)
        return carry

    lax.fori_loop(0, probes // (CHUNK * PLACED), body, jnp.zeros((count, LANES), BF16))


def scatter(rank_ref, coords_ref, slot_ref, block_ref, lane_ref, ids_ref, send_ref, acc_ref):
    probes = rank_ref.shape[1]
    many = ids_ref.shape[0]
    ids = twice(ids_ref[...])
    lane_ids = iota_bf16((PIECE, CHUNK))
    zero = jnp.zeros((), BF16)
    acc_ref[...] = jnp.zeros_like(acc_ref)

    def body(step, _):
        row_hots, lane_parts = [], []
        for g in range(GATHERED):
            at = chunk_at(step, g, GATHERED)
            rank, block, lane = rank_ref[:, at].astype(F32), block_ref[:, at], lane_ref[:, at]
            row_hots.append(
                jnp.concatenate(
                    [one_hot(ids, jnp.where(block == float(b), rank, -1.0)) for b in range(BLOCKS)], axis=0
                )
            )
            here = lane_ids == spread(lane, PIECE)
            high, low = [], []
            for v in range(3):
                value = coords_ref[v : v + 1, at]
                top = value.astype(BF16).astype(F32)
                high.append(top)
                low.append(value - top)
            high.append(slot_ref[:, at].astype(F32))
            chosen = [jnp.where(here, spread(part, PIECE), zero) for part in high + low]
            chosen.append(jnp.zeros((PIECE, CHUNK), BF16))
            lane_parts.append(jnp.concatenate(chosen, axis=0))
        acc_ref[...] += lax.dot_general(
            jnp.concatenate(row_hots, axis=1),
            jnp.concatenate(lane_parts, axis=1),
            (((1,), (1,)), ((), ())),
            preferred_element_type=F32,
        )
        return 0

    lax.fori_loop(0, probes // (GATHERED * CHUNK), body, 0)
    for b in range(BLOCKS):
        rows = slice(b * many, (b + 1) * many)
        send_ref[b] = acc_ref[rows, :LANES] + acc_ref[rows, LANES:]


def swap_groups(rows):
    lane = lax.broadcasted_iota(jnp.int32, (8, LANES), 1)
    for width in (2, 1):
        shift = width * PIECE
        lower = (lane // shift) % 2 == 0
        swapped = list(rows)
        for k in range(4):
            if (k // width) % 2 == 0:
                a, b = rows[k], rows[k + width]
                swapped[k] = jnp.where(lower, a, pltpu.roll(b, shift, 1))
                swapped[k + width] = jnp.where(lower, pltpu.roll(a, LANES - shift, 1), b)
        rows = swapped
    return rows


def write_nodes(nodes_ref):
    row = lax.broadcasted_iota(jnp.int32, (8, LANES), 0)
    for k in range(8):
        value = jnp.full((8, LANES), float(node_table[k, 0]), F32)
        for a in range(1, 8):
            value = jnp.where(row == a, float(node_table[k, a]), value)
        nodes_ref[8 * k : 8 * k + 8, :] = value


def turn_fields(fields_ref, spaced_ref, turned_ref):
    elements = fields_ref.shape[0]
    for k in range(fields_ref.shape[1] // LANES):
        spaced_ref[k * LANES : (k + 1) * LANES, :] = fields_ref[:, k * LANES : (k + 1) * LANES].astype(F32).T
    for c in range(8):
        turned_ref[:, c * elements : (c + 1) * elements] = spaced_ref[pl.ds(c, 256, stride=8), :].astype(BF16)


def lagrange(coord, nodes_ref):
    weight = nodes_ref[0:8, :]
    spread_coord = jnp.broadcast_to(coord, (8, LANES))
    for k in range(1, 8):
        weight = weight * (spread_coord - nodes_ref[8 * k : 8 * k + 8, :])
    return weight


def interpolate(rows, fields_ref, nodes_ref):
    depth = fields_ref.shape[1]
    elements = depth // 8
    zero = jnp.zeros((), BF16)
    ids = iota_bf16((16, LANES))
    pieces = [[] for _ in range(4)]
    for pair in range(len(rows[0]) // 2):
        weights, columns_of = [], []
        for j in range(2):
            r, s, t, slot = [row[2 * pair + j : 2 * pair + j + 1, :] for row in rows]
            weights.append((lagrange(r, nodes_ref), lagrange(s, nodes_ref)))
            weight_t = lagrange(t, nodes_ref)
            spread_t = [spread(weight_t[c : c + 1, :], 16) for c in range(8)]
            hots = [
                jnp.where(ids == spread(slot - float(16 * k), 16), jnp.ones((), BF16), zero)
                for k in range(elements // 16)
            ]
            columns_of.append(jnp.concatenate([hot * weight for weight in spread_t for hot in hots], axis=0))
        picker = jnp.concatenate(columns_of, axis=1)
        along = jnp.dot(fields_ref[...], picker, preferred_element_type=F32)
        for j in range(2):
            weight_r, weight_s = weights[j]
            columns = slice(j * LANES, (j + 1) * LANES)
            factors = [jnp.broadcast_to(weight_r[a : a + 1, :], (8, LANES)) for a in range(8)]
            for f in range(4):
                total = along[f * 64 : f * 64 + 8, columns] * factors[0]
                for a in range(1, 8):
                    total += along[f * 64 + a * 8 : f * 64 + a * 8 + 8, columns] * factors[a]
                pieces[f].append(jnp.sum(total * weight_s, axis=0, keepdims=True))
    return [jnp.concatenate(piece, axis=0) for piece in pieces]


def sample_kernel(
    sizes,
    rank_hbm,
    coords_hbm,
    slot_hbm,
    fields_hbm,
    part_ref,
    late_ref,
    block_ref,
    lane_ref,
    ids_ref,
    acc_ref,
    spaced_ref,
    turned_ref,
    table_ref,
    nodes_ref,
    rank_ref,
    coords_ref,
    slot_ref,
    fields_ref,
    back_ref,
    send_ref,
    recv_ref,
    values_ref,
    load_sem,
    out_sem,
    in_sem,
    back_out_sem,
    back_in_sem,
):
    count = sizes[0] * sizes[1] * sizes[2]
    quads, half = count // QUAD, count // 2
    me = (lax.axis_index("gx") * sizes[1] + lax.axis_index("gy")) * sizes[2] + lax.axis_index("gz")
    order = served(sizes)
    own = jnp.int32(0)
    for i in range(1, count):
        own = jnp.where(me == order[i], i, own)
    mesh_ids = pl.DeviceIdType.MESH

    def peer(i):
        rank = order[i]
        return (rank // (sizes[1] * sizes[2]), (rank // sizes[2]) % sizes[1], rank % sizes[2])

    def to_others(first, last, act):
        for i in range(first, last):
            pl.when(own != i)(functools.partial(act, i))

    def send(source, target, sent, arrived, i):
        pltpu.make_async_remote_copy(
            src_ref=source.at[:, i],
            dst_ref=target.at[:, own],
            send_sem=sent.at[0],
            recv_sem=arrived.at[own // QUAD],
            device_id=peer(i),
            device_id_type=mesh_ids,
        ).start()

    def keep(source, target, arrived):
        pltpu.make_async_copy(source.at[:, own], target.at[:, own], arrived.at[own // QUAD]).start()

    def wait_for(many, buffer, sem):
        pltpu.make_async_copy(buffer.at[:, :many], buffer.at[:, :many], sem).wait()

    loads = [
        pltpu.make_async_copy(source, target, load_sem.at[k])
        for k, (source, target) in enumerate(
            [(rank_hbm, rank_ref), (coords_hbm, coords_ref), (slot_hbm, slot_ref), (fields_hbm, fields_ref)]
        )
    ]
    for load in loads:
        load.start()
    barrier = pltpu.get_barrier_semaphore()
    to_others(
        0,
        count,
        lambda i: pl.semaphore_signal(barrier, inc=1, device_id=peer(i), device_id_type=mesh_ids),
    )
    for i in range(count):
        spaced_ref[i : i + 1, :] = jnp.full((1, LANES), float(order[i]), F32)
    ids_ref[...] = spaced_ref[:count, :].astype(BF16)
    write_nodes(nodes_ref)
    loads[0].wait()
    place(count, rank_ref, ids_ref, block_ref, lane_ref)
    loads[1].wait()
    loads[2].wait()
    scatter(rank_ref, coords_ref, slot_ref, block_ref, lane_ref, ids_ref, send_ref, acc_ref)
    pl.semaphore_wait(barrier, count - 1)

    def ask(phase, _):
        for h in range(2):

            @pl.when((phase + own // QUAD) % 2 == h)
            def _():
                to_others(h * half, (h + 1) * half, functools.partial(send, send_ref, recv_ref, out_sem, in_sem))

        return 0

    lax.fori_loop(0, 2, ask, 0)
    keep(send_ref, recv_ref, in_sem)
    loads[3].wait()
    turn_fields(fields_ref, spaced_ref, turned_ref)

    side = own // (count - QUAD)

    def body(step, _):
        quad = step + side * (step // 2) * (1 - 2 * (step % 2))
        wait_for(QUAD, recv_ref, in_sem.at[quad])
        for turn in range(5):
            spots = []
            for m in range(4):
                row = pl.multiple_of(quad * QUAD + 8 * (turn if turn < 4 else m), 8)
                spots.append((m if turn < 4 else 4, pl.ds(row, 8)))
            rows = swap_groups([recv_ref[b, at, :] for b, at in spots])
            values = swap_groups(interpolate(rows, turned_ref, nodes_ref))
            for (b, at), value in zip(spots, values):
                values_ref[b, at, :] = value

        for g in range(quads):

            @pl.when(quad == g)
            def _():
                to_others(
                    QUAD * g,
                    QUAD * g + QUAD,
                    functools.partial(send, values_ref, back_ref, back_out_sem, back_in_sem),
                )

        return 0

    lax.fori_loop(0, quads, body, 0)
    keep(values_ref, back_ref, back_in_sem)
    odd = own // QUAD % 2
    split = count - QUAD
    for flag, early, late in ((0, (0, split), (split, count)), (1, (split, count), (0, split))):

        @pl.when(odd == flag)
        def _():
            table = answers(early, back_ref, functools.partial(wait_for, QUAD), back_in_sem)
            table_ref[:, : table.shape[0]] = table.T.astype(BF16)
            pick(
                table_ref.at[:, : table.shape[0]], ids_ref[slice(*early), :], rank_ref, block_ref, lane_ref, None, part_ref
            )
            table = answers(late, back_ref, functools.partial(wait_for, QUAD), back_in_sem)
            late_ref[: table.shape[0], :] = table

    wait_for(count - 1, send_ref, out_sem.at[0])
    wait_for(count - 1, values_ref, back_out_sem.at[0])


def padded(many):
    return -(-BLOCKS * many // LANES) * LANES


def answers(span, back_ref, wait, back_in_sem):
    first, last = span
    for k in range(first // QUAD, last // QUAD):
        wait(back_ref, back_in_sem.at[k])
    rows = [back_ref[b, first:last, :] for b in range(BLOCKS)]
    rows.append(jnp.zeros((padded(last - first) - BLOCKS * (last - first), LANES), F32))
    return jnp.concatenate(rows, axis=0)


def pick(table_ref, ids, rank_ref, block_ref, lane_ref, part_ref, out_ref):
    probes = rank_ref.shape[1]
    ids = twice(ids)
    raised = ids + float(LANES)
    lane_ids = lax.broadcasted_iota(jnp.int32, (PIECE, CHUNK), 0).astype(F32)
    row_ids = lax.broadcasted_iota(jnp.int32, (8, CHUNK), 0)

    def merge(a, b, shift):
        lower = (row_ids // shift) % 2 == 0
        return jnp.where(lower, a, b) + pltpu.roll(jnp.where(lower, b, a), shift, 0)

    def body(step, _):
        for g in range(RETURNED):
            at = chunk_at(step, g, RETURNED)
            rank, block = rank_ref[:, at].astype(F32), block_ref[:, at]
            code = rank + block * float(LANES)
            hots = []
            for b in range(0, BLOCKS, 2):
                inside = (block >= float(b)) & (block < float(b + 2))
                row = jnp.where(inside, code - float(b * LANES), -1.0)
                hots += [one_hot(known, row) for known in (ids, raised)[: BLOCKS - b]]
            spare = table_ref.shape[1] - BLOCKS * ids.shape[0]
            if spare:
                hots.append(jnp.zeros((spare, CHUNK), BF16))
            picked = jnp.dot(table_ref[...], jnp.concatenate(hots, axis=0), preferred_element_type=F32)
            here = lane_ids == jnp.broadcast_to(lane_ref[:, at], (PIECE, CHUNK))
            sums = []
            for f in range(4):
                chosen = jnp.where(here, picked[f * PIECE : (f + 1) * PIECE], 0.0)
                sums.append(sum(chosen[8 * k : 8 * k + 8] for k in range(PIECE // 8)))
            mixed = merge(merge(sums[0], sums[1], 1), merge(sums[2], sums[3], 1), 2)
            value = (mixed + pltpu.roll(mixed, 4, 0))[:4]
            out_ref[:, at] = value if part_ref is None else value + part_ref[:, at]
        return 0

    lax.fori_loop(0, probes // (RETURNED * CHUNK), body, 0)


def return_kernel(sizes, late_ref, part_ref, rank_ref, block_ref, lane_ref, ids_ref, out_ref, table_ref):
    count = ids_ref.shape[0]
    own = (lax.axis_index("gx") * sizes[1] + lax.axis_index("gy")) * sizes[2] + lax.axis_index("gz")
    odd = jnp.int32(0)
    for i, rank in enumerate(served(sizes)):
        odd = jnp.where(own == rank, i // QUAD % 2, odd)
    split = count - QUAD
    for flag, (first, last) in enumerate(((split, count), (0, split))):

        @pl.when(odd == flag)
        def _():
            rows = padded(last - first)
            table_ref[:, :rows] = late_ref[:rows, :].T.astype(BF16)
            pick(table_ref.at[:, :rows], ids_ref[first:last, :], rank_ref, block_ref, lane_ref, part_ref, out_ref)


VMEM = pl.BlockSpec(memory_space=pltpu.VMEM)
HBM = pl.BlockSpec(memory_space=pltpu.HBM)


def call(kernel, inputs, outputs, scratch, **options):
    return pl.pallas_call(
        kernel,
        out_shape=outputs,
        in_specs=inputs,
        out_specs=jax.tree.map(lambda _: VMEM, outputs),
        scratch_shapes=scratch,
        compiler_params=pltpu.CompilerParams(vmem_limit_bytes=48 << 20, **options),
    )


def local(sizes, fields, coordinates, element_rank, element_slot):
    count = sizes[0] * sizes[1] * sizes[2]
    probes = element_slot.shape[0]
    elements = fields.shape[0]
    line = jax.ShapeDtypeStruct((1, probes), F32)

    buffer = pltpu.VMEM((BLOCKS, count, LANES), F32)
    rank = element_rank.reshape(1, probes)
    late = padded(count - QUAD)
    whole = jax.ShapeDtypeStruct((4, probes), F32)
    part, returned, block, lane, ids = call(
        functools.partial(sample_kernel, sizes),
        [HBM] * 4,
        (
            whole,
            jax.ShapeDtypeStruct((late, LANES), F32),
            line,
            line,
            jax.ShapeDtypeStruct((count, LANES), BF16),
        ),
        [
            pltpu.VMEM((BLOCKS * count, 2 * LANES), F32),
            pltpu.VMEM((256 * 8, elements), F32),
            pltpu.VMEM((256, 8 * elements), BF16),
            pltpu.VMEM((LANES, late), BF16),
        ]
        + [
            pltpu.VMEM((64, LANES), F32),
            pltpu.VMEM(rank.shape, jnp.int32),
            pltpu.VMEM(coordinates.shape, F32),
            pltpu.VMEM(rank.shape, jnp.int32),
            pltpu.VMEM(fields.shape, BF16),
        ]
        + [buffer] * 4
        + [pltpu.SemaphoreType.DMA((n,)) for n in (4, 1, count // QUAD, 1, count // QUAD)],
        collective_id=0,
        has_side_effects=True,
    )(
        *[
            pltpu.with_memory_space_constraint(array, pltpu.HBM)
            for array in (rank, coordinates, element_slot.reshape(1, probes), fields)
        ]
    )
    return call(
        functools.partial(return_kernel, sizes),
        [VMEM] * 6,
        whole,
        [pltpu.VMEM((LANES, late), BF16)],
    )(returned, part, rank, block, lane, ids)


def solution(mesh):
    sizes = tuple(mesh.shape[axis] for axis in AXES)
    placed = (P(AXES, None), P(None, AXES), P(AXES, None), P(AXES))
    return jax.shard_map(
        functools.partial(local, sizes),
        mesh=mesh,
        in_specs=placed,
        out_specs=P(None, AXES),
        check_vma=False,
    )
```

```python
import functools

import jax
import jax.numpy as jnp
import numpy as np
from jax import lax
from jax.experimental import pallas as pl
from jax.experimental.pallas import tpu as pltpu
from jax.sharding import PartitionSpec as P

AXES = ("gx", "gy", "gz")
F32, BF16 = jnp.float32, jnp.bfloat16
LANES = 128
CHUNK = 256
PIECE = 32
BLOCKS = 5
QUAD = 32
PLACED = 32
GATHERED = 32
RETURNED = 32

gll_points = np.array(
    [
        -1.0,
        -0.8717401485096066,
        -0.5917001814331423,
        -0.2092992179024789,
        0.2092992179024789,
        0.5917001814331423,
        0.8717401485096066,
        1.0,
    ]
)
gll_scale = np.array(
    [1.0 / np.prod([gll_points[a] - gll_points[b] for b in range(8) if b != a]) for a in range(8)]
)
node_table = np.stack([gll_scale] + [np.roll(gll_points, -k) for k in range(1, 8)], axis=0)

REACHED = ((0.0, 1.1, 1.2, 1.6), (0.0, 1.3, 1.5, 1.8), (0.0, 1.5, 2.3, 2.8))


def served(sizes):
    def reached(rank):
        x, y, z = rank // (sizes[1] * sizes[2]), (rank // sizes[2]) % sizes[1], rank % sizes[2] // 2
        return REACHED[0][x] + REACHED[1][y] + REACHED[2][z]

    return sorted(range(sizes[0] * sizes[1] * sizes[2]), key=lambda rank: (reached(rank), rank))


def iota_bf16(shape):
    return lax.broadcasted_iota(jnp.int32, shape, 0).astype(F32).astype(BF16)


def spread(row, count):
    return jnp.broadcast_to(row, (count, row.shape[1])).astype(BF16)


def one_hot(ids, row):
    return jnp.where(ids == spread(row, ids.shape[0]), jnp.ones((), BF16), jnp.zeros((), BF16))


def twice(ids):
    return jnp.concatenate([ids, ids], axis=1)


def chunk_at(step, g, group):
    return pl.ds(pl.multiple_of((step * group + g) * CHUNK, CHUNK), CHUNK)


def place(count, rank_ref, ids_ref, block_ref, lane_ref):
    probes = rank_ref.shape[1]
    ids = twice(ids_ref[...])
    before = lax.broadcasted_iota(jnp.int32, (CHUNK, CHUNK), 0) <= lax.broadcasted_iota(jnp.int32, (CHUNK, CHUNK), 1)
    prefix = jnp.where(before, 1.0, 0.0).astype(BF16)

    def body(step, carry):
        hots = [one_hot(ids, rank_ref[:, chunk_at(step, g, PLACED)].astype(F32)) for g in range(PLACED)]
        counted = jnp.dot(jnp.concatenate(hots, axis=0), prefix, preferred_element_type=F32)
        for g in range(PLACED):
            at = chunk_at(step, g, PLACED)
            piece = counted[g * count : (g + 1) * count].astype(BF16)
            inside = (piece + twice(carry)) * hots[g]
            total = inside[:16]
            for k in range(1, count // 16):
                total = total + inside[16 * k : 16 * k + 16]
            position = jnp.sum(total.astype(F32), axis=0, keepdims=True) - 1.0
            block = jnp.floor(position * (1.0 / PIECE))
            lane_ref[:, at] = position - block * PIECE
            block_ref[:, at] = block
            carry = carry + jnp.broadcast_to(piece[:, CHUNK - 1 :], carry.shape)
        return carry

    lax.fori_loop(0, probes // (CHUNK * PLACED), body, jnp.zeros((count, LANES), BF16))


def scatter(rank_ref, coords_ref, slot_ref, block_ref, lane_ref, ids_ref, send_ref, acc_ref):
    probes = rank_ref.shape[1]
    many = ids_ref.shape[0]
    ids = twice(ids_ref[...])
    lane_ids = iota_bf16((PIECE, CHUNK))
    zero = jnp.zeros((), BF16)
    acc_ref[...] = jnp.zeros_like(acc_ref)

    def body(step, _):
        row_hots, lane_parts = [], []
        for g in range(GATHERED):
            at = chunk_at(step, g, GATHERED)
            rank, block, lane = rank_ref[:, at].astype(F32), block_ref[:, at], lane_ref[:, at]
            row_hots.append(
                jnp.concatenate(
                    [one_hot(ids, jnp.where(block == float(b), rank, -1.0)) for b in range(BLOCKS)], axis=0
                )
            )
            here = lane_ids == spread(lane, PIECE)
            high, low = [], []
            for v in range(3):
                value = coords_ref[v : v + 1, at]
                top = value.astype(BF16).astype(F32)
                high.append(top)
                low.append(value - top)
            high.append(slot_ref[:, at].astype(F32))
            chosen = [jnp.where(here, spread(part, PIECE), zero) for part in high + low]
            chosen.append(jnp.zeros((PIECE, CHUNK), BF16))
            lane_parts.append(jnp.concatenate(chosen, axis=0))
        acc_ref[...] += lax.dot_general(
            jnp.concatenate(row_hots, axis=1),
            jnp.concatenate(lane_parts, axis=1),
            (((1,), (1,)), ((), ())),
            preferred_element_type=F32,
        )
        return 0

    lax.fori_loop(0, probes // (GATHERED * CHUNK), body, 0)
    for b in range(BLOCKS):
        rows = slice(b * many, (b + 1) * many)
        send_ref[b] = acc_ref[rows, :LANES] + acc_ref[rows, LANES:]


def swap_groups(rows):
    lane = lax.broadcasted_iota(jnp.int32, (8, LANES), 1)
    for width in (2, 1):
        shift = width * PIECE
        lower = (lane // shift) % 2 == 0
        swapped = list(rows)
        for k in range(4):
            if (k // width) % 2 == 0:
                a, b = rows[k], rows[k + width]
                swapped[k] = jnp.where(lower, a, pltpu.roll(b, shift, 1))
                swapped[k + width] = jnp.where(lower, pltpu.roll(a, LANES - shift, 1), b)
        rows = swapped
    return rows


def write_nodes(nodes_ref):
    row = lax.broadcasted_iota(jnp.int32, (8, LANES), 0)
    for k in range(8):
        value = jnp.full((8, LANES), float(node_table[k, 0]), F32)
        for a in range(1, 8):
            value = jnp.where(row == a, float(node_table[k, a]), value)
        nodes_ref[8 * k : 8 * k + 8, :] = value


def turn_fields(fields_ref, spaced_ref, turned_ref):
    elements = fields_ref.shape[0]
    for k in range(fields_ref.shape[1] // LANES):
        spaced_ref[k * LANES : (k + 1) * LANES, :] = fields_ref[:, k * LANES : (k + 1) * LANES].astype(F32).T
    for c in range(8):
        turned_ref[:, c * elements : (c + 1) * elements] = spaced_ref[pl.ds(c, 256, stride=8), :].astype(BF16)


def lagrange(coord, nodes_ref):
    weight = nodes_ref[0:8, :]
    spread_coord = jnp.broadcast_to(coord, (8, LANES))
    for k in range(1, 8):
        weight = weight * (spread_coord - nodes_ref[8 * k : 8 * k + 8, :])
    return weight


def interpolate(rows, fields_ref, nodes_ref):
    depth = fields_ref.shape[1]
    elements = depth // 8
    zero = jnp.zeros((), BF16)
    ids = iota_bf16((16, LANES))
    pieces = [[] for _ in range(4)]
    for pair in range(len(rows[0]) // 2):
        weights, columns_of = [], []
        for j in range(2):
            r, s, t, slot = [row[2 * pair + j : 2 * pair + j + 1, :] for row in rows]
            weights.append((lagrange(r, nodes_ref), lagrange(s, nodes_ref)))
            weight_t = lagrange(t, nodes_ref)
            spread_t = [spread(weight_t[c : c + 1, :], 16) for c in range(8)]
            hots = [
                jnp.where(ids == spread(slot - float(16 * k), 16), jnp.ones((), BF16), zero)
                for k in range(elements // 16)
            ]
            columns_of.append(jnp.concatenate([hot * weight for weight in spread_t for hot in hots], axis=0))
        picker = jnp.concatenate(columns_of, axis=1)
        along = jnp.dot(fields_ref[...], picker, preferred_element_type=F32)
        for j in range(2):
            weight_r, weight_s = weights[j]
            columns = slice(j * LANES, (j + 1) * LANES)
            factors = [jnp.broadcast_to(weight_r[a : a + 1, :], (8, LANES)) for a in range(8)]
            for f in range(4):
                total = along[f * 64 : f * 64 + 8, columns] * factors[0]
                for a in range(1, 8):
                    total += along[f * 64 + a * 8 : f * 64 + a * 8 + 8, columns] * factors[a]
                pieces[f].append(jnp.sum(total * weight_s, axis=0, keepdims=True))
    return [jnp.concatenate(piece, axis=0) for piece in pieces]


def sample_kernel(
    sizes,
    rank_hbm,
    coords_hbm,
    slot_hbm,
    fields_hbm,
    part_ref,
    late_ref,
    block_ref,
    lane_ref,
    ids_ref,
    acc_ref,
    spaced_ref,
    turned_ref,
    table_ref,
    nodes_ref,
    rank_ref,
    coords_ref,
    slot_ref,
    fields_ref,
    back_ref,
    send_ref,
    recv_ref,
    values_ref,
    load_sem,
    out_sem,
    in_sem,
    back_out_sem,
    back_in_sem,
):
    count = sizes[0] * sizes[1] * sizes[2]
    quads, half = count // QUAD, count // 2
    me = (lax.axis_index("gx") * sizes[1] + lax.axis_index("gy")) * sizes[2] + lax.axis_index("gz")
    order = served(sizes)
    own = jnp.int32(0)
    for i in range(1, count):
        own = jnp.where(me == order[i], i, own)
    mesh_ids = pl.DeviceIdType.MESH

    def peer(i):
        rank = order[i]
        return (rank // (sizes[1] * sizes[2]), (rank // sizes[2]) % sizes[1], rank % sizes[2])

    def to_others(first, last, act):
        for i in range(first, last):
            pl.when(own != i)(functools.partial(act, i))

    def send(source, target, sent, arrived, i):
        pltpu.make_async_remote_copy(
            src_ref=source.at[:, i],
            dst_ref=target.at[:, own],
            send_sem=sent.at[0],
            recv_sem=arrived.at[own // QUAD],
            device_id=peer(i),
            device_id_type=mesh_ids,
        ).start()

    def keep(source, target, arrived):
        pltpu.make_async_copy(source.at[:, own], target.at[:, own], arrived.at[own // QUAD]).start()

    def wait_for(many, buffer, sem):
        pltpu.make_async_copy(buffer.at[:, :many], buffer.at[:, :many], sem).wait()

    loads = [
        pltpu.make_async_copy(source, target, load_sem.at[k])
        for k, (source, target) in enumerate(
            [(rank_hbm, rank_ref), (coords_hbm, coords_ref), (slot_hbm, slot_ref), (fields_hbm, fields_ref)]
        )
    ]
    for load in loads:
        load.start()
    barrier = pltpu.get_barrier_semaphore()
    to_others(
        0,
        count,
        lambda i: pl.semaphore_signal(barrier, inc=1, device_id=peer(i), device_id_type=mesh_ids),
    )
    for i in range(count):
        spaced_ref[i : i + 1, :] = jnp.full((1, LANES), float(order[i]), F32)
    ids_ref[...] = spaced_ref[:count, :].astype(BF16)
    write_nodes(nodes_ref)
    loads[0].wait()
    place(count, rank_ref, ids_ref, block_ref, lane_ref)
    loads[1].wait()
    loads[2].wait()
    scatter(rank_ref, coords_ref, slot_ref, block_ref, lane_ref, ids_ref, send_ref, acc_ref)
    pl.semaphore_wait(barrier, count - 1)

    def ask(phase, _):
        for h in range(2):

            @pl.when((phase + (own // QUAD + 1) // 2 + 1) % 2 == h)
            def _():
                to_others(h * half, (h + 1) * half, functools.partial(send, send_ref, recv_ref, out_sem, in_sem))

        return 0

    lax.fori_loop(0, 2, ask, 0)
    keep(send_ref, recv_ref, in_sem)
    loads[3].wait()
    turn_fields(fields_ref, spaced_ref, turned_ref)

    side = own // (count - QUAD)

    def body(step, _):
        quad = step + side * (step // 2) * (1 - 2 * (step % 2))
        wait_for(QUAD, recv_ref, in_sem.at[quad])
        for turn in range(5):
            spots = []
            for m in range(4):
                row = pl.multiple_of(quad * QUAD + 8 * (turn if turn < 4 else m), 8)
                spots.append((m if turn < 4 else 4, pl.ds(row, 8)))
            rows = swap_groups([recv_ref[b, at, :] for b, at in spots])
            values = swap_groups(interpolate(rows, turned_ref, nodes_ref))
            for (b, at), value in zip(spots, values):
                values_ref[b, at, :] = value

        for g in range(quads):

            @pl.when(quad == g)
            def _():
                to_others(
                    QUAD * g,
                    QUAD * g + QUAD,
                    functools.partial(send, values_ref, back_ref, back_out_sem, back_in_sem),
                )

        return 0

    lax.fori_loop(0, quads, body, 0)
    keep(values_ref, back_ref, back_in_sem)
    odd = own // QUAD % 2
    split = count - QUAD
    for flag, early, late in ((0, (0, split), (split, count)), (1, (split, count), (0, split))):

        @pl.when(odd == flag)
        def _():
            table = answers(early, back_ref, functools.partial(wait_for, QUAD), back_in_sem)
            table_ref[:, : table.shape[0]] = table.T.astype(BF16)
            pick(
                table_ref.at[:, : table.shape[0]], ids_ref[slice(*early), :], rank_ref, block_ref, lane_ref, None, part_ref
            )
            table = answers(late, back_ref, functools.partial(wait_for, QUAD), back_in_sem)
            late_ref[: table.shape[0], :] = table

    wait_for(count - 1, send_ref, out_sem.at[0])
    wait_for(count - 1, values_ref, back_out_sem.at[0])


def padded(many):
    return -(-BLOCKS * many // LANES) * LANES


def answers(span, back_ref, wait, back_in_sem):
    first, last = span
    for k in range(first // QUAD, last // QUAD):
        wait(back_ref, back_in_sem.at[k])
    rows = [back_ref[b, first:last, :] for b in range(BLOCKS)]
    rows.append(jnp.zeros((padded(last - first) - BLOCKS * (last - first), LANES), F32))
    return jnp.concatenate(rows, axis=0)


def pick(table_ref, ids, rank_ref, block_ref, lane_ref, part_ref, out_ref):
    probes = rank_ref.shape[1]
    ids = twice(ids)
    raised = ids + float(LANES)
    lane_ids = lax.broadcasted_iota(jnp.int32, (PIECE, CHUNK), 0).astype(F32)
    row_ids = lax.broadcasted_iota(jnp.int32, (8, CHUNK), 0)

    def merge(a, b, shift):
        lower = (row_ids // shift) % 2 == 0
        return jnp.where(lower, a, b) + pltpu.roll(jnp.where(lower, b, a), shift, 0)

    def body(step, _):
        for g in range(RETURNED):
            at = chunk_at(step, g, RETURNED)
            rank, block = rank_ref[:, at].astype(F32), block_ref[:, at]
            code = rank + block * float(LANES)
            hots = []
            for b in range(0, BLOCKS, 2):
                inside = (block >= float(b)) & (block < float(b + 2))
                row = jnp.where(inside, code - float(b * LANES), -1.0)
                hots += [one_hot(known, row) for known in (ids, raised)[: BLOCKS - b]]
            spare = table_ref.shape[1] - BLOCKS * ids.shape[0]
            if spare:
                hots.append(jnp.zeros((spare, CHUNK), BF16))
            picked = jnp.dot(table_ref[...], jnp.concatenate(hots, axis=0), preferred_element_type=F32)
            here = lane_ids == jnp.broadcast_to(lane_ref[:, at], (PIECE, CHUNK))
            sums = []
            for f in range(4):
                chosen = jnp.where(here, picked[f * PIECE : (f + 1) * PIECE], 0.0)
                sums.append(sum(chosen[8 * k : 8 * k + 8] for k in range(PIECE // 8)))
            mixed = merge(merge(sums[0], sums[1], 1), merge(sums[2], sums[3], 1), 2)
            value = (mixed + pltpu.roll(mixed, 4, 0))[:4]
            out_ref[:, at] = value if part_ref is None else value + part_ref[:, at]
        return 0

    lax.fori_loop(0, probes // (RETURNED * CHUNK), body, 0)


def return_kernel(sizes, late_ref, part_ref, rank_ref, block_ref, lane_ref, ids_ref, out_ref, table_ref):
    count = ids_ref.shape[0]
    own = (lax.axis_index("gx") * sizes[1] + lax.axis_index("gy")) * sizes[2] + lax.axis_index("gz")
    odd = jnp.int32(0)
    for i, rank in enumerate(served(sizes)):
        odd = jnp.where(own == rank, i // QUAD % 2, odd)
    split = count - QUAD
    for flag, (first, last) in enumerate(((split, count), (0, split))):

        @pl.when(odd == flag)
        def _():
            rows = padded(last - first)
            table_ref[:, :rows] = late_ref[:rows, :].T.astype(BF16)
            pick(table_ref.at[:, :rows], ids_ref[first:last, :], rank_ref, block_ref, lane_ref, part_ref, out_ref)


VMEM = pl.BlockSpec(memory_space=pltpu.VMEM)
HBM = pl.BlockSpec(memory_space=pltpu.HBM)


def call(kernel, inputs, outputs, scratch, **options):
    return pl.pallas_call(
        kernel,
        out_shape=outputs,
        in_specs=inputs,
        out_specs=jax.tree.map(lambda _: VMEM, outputs),
        scratch_shapes=scratch,
        compiler_params=pltpu.CompilerParams(vmem_limit_bytes=48 << 20, **options),
    )


def local(sizes, fields, coordinates, element_rank, element_slot):
    count = sizes[0] * sizes[1] * sizes[2]
    probes = element_slot.shape[0]
    elements = fields.shape[0]
    line = jax.ShapeDtypeStruct((1, probes), F32)

    buffer = pltpu.VMEM((BLOCKS, count, LANES), F32)
    rank = element_rank.reshape(1, probes)
    late = padded(count - QUAD)
    whole = jax.ShapeDtypeStruct((4, probes), F32)
    part, returned, block, lane, ids = call(
        functools.partial(sample_kernel, sizes),
        [HBM] * 4,
        (
            whole,
            jax.ShapeDtypeStruct((late, LANES), F32),
            line,
            line,
            jax.ShapeDtypeStruct((count, LANES), BF16),
        ),
        [
            pltpu.VMEM((BLOCKS * count, 2 * LANES), F32),
            pltpu.VMEM((256 * 8, elements), F32),
            pltpu.VMEM((256, 8 * elements), BF16),
            pltpu.VMEM((LANES, late), BF16),
        ]
        + [
            pltpu.VMEM((64, LANES), F32),
            pltpu.VMEM(rank.shape, jnp.int32),
            pltpu.VMEM(coordinates.shape, F32),
            pltpu.VMEM(rank.shape, jnp.int32),
            pltpu.VMEM(fields.shape, BF16),
        ]
        + [buffer] * 4
        + [pltpu.SemaphoreType.DMA((n,)) for n in (4, 1, count // QUAD, 1, count // QUAD)],
        collective_id=0,
        has_side_effects=True,
    )(
        *[
            pltpu.with_memory_space_constraint(array, pltpu.HBM)
            for array in (rank, coordinates, element_slot.reshape(1, probes), fields)
        ]
    )
    return call(
        functools.partial(return_kernel, sizes),
        [VMEM] * 6,
        whole,
        [pltpu.VMEM((LANES, late), BF16)],
    )(returned, part, rank, block, lane, ids)


def solution(mesh):
    sizes = tuple(mesh.shape[axis] for axis in AXES)
    placed = (P(AXES, None), P(None, AXES), P(AXES, None), P(AXES))
    return jax.shard_map(
        functools.partial(local, sizes),
        mesh=mesh,
        in_specs=placed,
        out_specs=P(None, AXES),
        check_vma=False,
    )
```
